256 devices in a mesh: row: 32 (over y, z_hi, core), col: 8 (over z_lo, x).
Axes of the slice: x: 4, y: 4, z: 8 (z_hi: 4, z_lo: 2; z = z_hi * 2 + z_lo), core: 2. Of those that a mesh axis runs over, the one named last changes fastest.
Arguments:
- alignment: bfloat16 [64, 1024, 64], P(None, ('col', 'row')), may hold values from -6 to 6
- pair_rep: bfloat16 [1024, 1024, 128], P('row', 'col'), may hold values from -128 to 128
- outer_left: bfloat16 [64, 32], replicated, may hold values from -0.75 to 0.75
- outer_right: bfloat16 [64, 32], replicated, may hold values from -0.75 to 0.75
- outer_proj: bfloat16 [1024, 128], replicated, may hold values from -1.5 to 1.5
- outer_bias: float32 [128], replicated, may hold values from -3 to 3
- average_value: bfloat16 [64, 256], replicated, may hold values from -0.75 to 0.75
- average_gate: bfloat16 [64, 256], replicated, may hold values from -0.75 to 0.75
- average_logit: bfloat16 [128, 8], replicated, may hold values from -28 to 28
- average_out: bfloat16 [256, 64], replicated, may hold values from -1 to 1
- triangle_proj: bfloat16 [128, 512], replicated, may hold values from -0.5 to 0.5
- triangle_bias: bfloat16 [128, 4], replicated, may hold values from -0.5 to 0.5
Outputs:
- pair_new: bfloat16 [1024, 1024, 128], P('row', 'col')
- alignment_update: bfloat16 [64, 1024, 64], P(None, ('row', 'col'))
- triangle_inputs: bfloat16 [1024, 1024, 512], P(('col', 'row'))
- edge_bias: bfloat16 [4, 1024, 1024], P(None, ('col', 'row'))
The draws below stay inside these ranges and needn't reach their ends.
All inputs are finite; a program needn't handle non-finite values.
Results may differ from the reference program's by a relative error of at most 0.02.
The reference program's roundings to bfloat16 on the way count: a program that leaves them out, or rounds other values in their place, can miss the bound.
Values may be sent and summed in bfloat16 or wider, within the bound.
No kernel may reach another device: no remote copies, remote signals or barrier semaphores. Data moves between devices by JAX's collectives and lax.ppermute only.
A program may use at most 64 MiB of HBM per device.

```python
import math
import jax
import jax.numpy as jnp
from jax import lax

CM = 64
CZ = 128
OPM_C = 32
PWA_H = 8
PWA_C = 32
TRI_H = 4
TRI_C = 32
SEQS = 64
ROW_TOK = 32
TOKENS = 1024
N_ROW = 32


def draw_average_logit(key, part):
    strength = jnp.exp(jax.random.uniform(jax.random.fold_in(key, 102), (PWA_H,), jnp.float32, math.log(0.7), math.log(4.0)))
    noise_part = jax.random.normal(jax.random.fold_in(key, 103), (CZ, PWA_H), jnp.float32)
    return (noise_part * strength[None, :] / math.sqrt(CZ)).astype(jnp.bfloat16)


def draw_pair_rep(key, part):
    noise_part = jnp.clip(jax.random.normal(jax.random.fold_in(key, 201), (TOKENS, TOKENS, CZ), jnp.float32), -6.0, 6.0)
    return noise_part.astype(jnp.bfloat16)


def block_scale(key, extent, pieces, low, high):
    gain = 1.0
    for dim, shards_of in pieces:
        heights = jax.random.uniform(jax.random.fold_in(jax.random.fold_in(key, 6), dim), (shards_of,), jnp.float32, low / len(pieces), high / len(pieces))
        gain = gain * jnp.repeat(jnp.exp(heights), extent[dim] // shards_of).reshape((-1,) + (1,) * (len(extent) - 1 - dim))
    return gain


def scatter_about(key, dims, width, most, cuts=(), kind=jnp.bfloat16):
    array = width * jax.random.normal(key, dims, jnp.float32)
    if cuts:
        array = array * block_scale(key, dims, cuts, -0.22, 0.18)
    return jnp.clip(array, -most, most).astype(kind)


def setup_inputs(seed: int = 0) -> dict:
    key_list = jax.random.split(jax.random.key(seed), 13)
    alignment = scatter_about(key_list[0], (SEQS, TOKENS, CM), 1.0, 6.0, ((1, 256),))
    pair_rep = draw_pair_rep(jax.random.fold_in(key_list[12], 71), 0)
    outer_left = scatter_about(key_list[2], (CM, OPM_C), CM ** -0.5, 0.75)
    outer_right = scatter_about(key_list[3], (CM, OPM_C), CM ** -0.5, 0.75)
    outer_proj = scatter_about(key_list[4], (OPM_C * OPM_C, CZ), (OPM_C * OPM_C // SEQS) ** -0.5, 1.5)
    outer_bias = scatter_about(key_list[5], (CZ,), 0.5, 3.0, (), jnp.float32)
    average_value = scatter_about(key_list[6], (CM, PWA_H * PWA_C), CM ** -0.5, 0.75)
    average_gate = scatter_about(key_list[7], (CM, PWA_H * PWA_C), CM ** -0.5, 0.75)
    average_logit = draw_average_logit(jax.random.fold_in(key_list[12], 71), 0)
    average_out = scatter_about(key_list[9], (PWA_H * PWA_C, CM), PWA_C ** -0.5, 1.0)
    triangle_proj = scatter_about(key_list[10], (CZ, 4 * TRI_H * TRI_C), CZ ** -0.5, 0.5)
    triangle_bias = scatter_about(key_list[11], (CZ, TRI_H), CZ ** -0.5, 0.5)
    return {"alignment": alignment, "pair_rep": pair_rep, "outer_left": outer_left, "outer_right": outer_right, "outer_proj": outer_proj, "outer_bias": outer_bias, "average_value": average_value, "average_gate": average_gate, "average_logit": average_logit, "average_out": average_out, "triangle_proj": triangle_proj, "triangle_bias": triangle_bias}


def standardize(values):
    widened = values.astype(jnp.float32)
    centered = widened - lax.optimization_barrier(jnp.mean(widened, axis=-1, keepdims=True))
    spread = lax.optimization_barrier(jnp.mean(centered * centered, axis=-1, keepdims=True))
    return centered * lax.rsqrt(spread + 1e-05)

def reference(alignment, pair_rep, outer_left, outer_right, outer_proj, outer_bias, average_value, average_gate, average_logit, average_out, triangle_proj, triangle_bias):
    alignment_layer_norm = standardize(alignment).astype(jnp.bfloat16)
    left_factor = jnp.dot(alignment_layer_norm, outer_left, preferred_element_type=jnp.float32).astype(jnp.bfloat16)
    right_factor = jnp.dot(alignment_layer_norm, outer_right, preferred_element_type=jnp.float32).astype(jnp.bfloat16)
    right_wide = right_factor.astype(jnp.float32)
    left_blocks = jnp.transpose(left_factor.reshape(SEQS, N_ROW, ROW_TOK, OPM_C), (1, 0, 2, 3))
    pair_blocks = pair_rep.reshape(N_ROW, ROW_TOK, TOKENS, CZ)

    def pair_block(block_items):
        left_block, pair_rows = block_items
        outer_mean = jnp.einsum('sic,sjd->ijcd', left_block.astype(jnp.float32), right_wide) / SEQS
        outer_mean = outer_mean.reshape(ROW_TOK, TOKENS, OPM_C * OPM_C).astype(jnp.bfloat16)
        update = jnp.dot(outer_mean, outer_proj, preferred_element_type=jnp.float32)
        return (pair_rows.astype(jnp.float32) + update + outer_bias).astype(jnp.bfloat16)
    pair_new = lax.map(pair_block, (left_blocks, pair_blocks)).reshape(TOKENS, TOKENS, CZ)
    pair_norm = standardize(pair_new).astype(jnp.bfloat16)
    logits = jnp.dot(pair_norm, average_logit, preferred_element_type=jnp.float32)
    weights = jnp.exp(logits - lax.optimization_barrier(jnp.max(logits, axis=1, keepdims=True))).astype(jnp.bfloat16)
    weights_wide = weights.astype(jnp.float32)
    denom = lax.optimization_barrier(jnp.sum(weights_wide, axis=1))
    values = jnp.dot(alignment_layer_norm, average_value, preferred_element_type=jnp.float32).astype(jnp.bfloat16)
    values = values.reshape(SEQS, TOKENS, PWA_H, PWA_C)
    gate_vals = jax.nn.sigmoid(jnp.dot(alignment_layer_norm, average_gate, preferred_element_type=jnp.float32))
    gate_vals = gate_vals.reshape(SEQS, TOKENS, PWA_H, PWA_C)
    numer = jnp.einsum('ijh,sjhc->sihc', weights_wide, values.astype(jnp.float32))
    gated = (gate_vals * numer / denom[None, :, :, None]).reshape(SEQS, TOKENS, PWA_H * PWA_C)
    alignment_update = jnp.dot(gated, average_out.astype(jnp.float32), precision=lax.Precision.HIGHEST).astype(jnp.bfloat16)
    turned = jnp.swapaxes(pair_norm, 0, 1).reshape(N_ROW, ROW_TOK, TOKENS, CZ)
    split_at = 3 * TRI_H * TRI_C

    def triangle_block(block_rows):
        projected = jnp.dot(block_rows, triangle_proj, preferred_element_type=jnp.float32)
        inputs = jnp.concatenate([projected[..., :split_at], jax.nn.sigmoid(projected[..., split_at:])], axis=-1).astype(jnp.bfloat16)
        bias_rows = jnp.dot(block_rows, triangle_bias, preferred_element_type=jnp.float32).astype(jnp.bfloat16)
        return (inputs, bias_rows)
    triangle_blocks, bias_blocks = lax.map(triangle_block, turned)
    triangle_inputs = triangle_blocks.reshape(TOKENS, TOKENS, 4 * TRI_H * TRI_C)
    edge_bias = jnp.transpose(bias_blocks.reshape(TOKENS, TOKENS, TRI_H), (2, 0, 1))
    return (pair_new, alignment_update, triangle_inputs, edge_bias)
```

```python
import functools

import jax
import jax.numpy as jnp
from jax import lax
from jax.experimental import pallas as pl
from jax.experimental.pallas import tpu as pltpu
from jax.sharding import Mesh, PartitionSpec as P


BF16 = jnp.bfloat16
F32 = jnp.float32
ROW = ("y", "zh", "co")
COL = ("zl", "x")
ALL = ROW + COL


def dot(a, b):
    return jnp.dot(a, b, preferred_element_type=F32)


def dot_nt(a, b):
    return lax.dot_general(a, b, (((1,), (1,)), ((), ())), preferred_element_type=F32)


def cost(flops, nbytes, trans=0):
    return pl.CostEstimate(flops=flops, bytes_accessed=nbytes, transcendentals=trans)


def standardize(values):
    widened = values.astype(F32)
    centered = widened - jnp.mean(widened, axis=-1, keepdims=True)
    spread = jnp.mean(centered * centered, axis=-1, keepdims=True)
    return centered * lax.rsqrt(spread + 1e-05)


def pair_kernel(
    right_ref, left_ref, pair_ref, proj_ref, bias_ref, logit_w_ref,
    new_ref, turned_ref, logit_ref, stack, plane, turn,
):
    groups = 8
    rows = pair_ref.shape[0]

    @pl.when(pl.program_id(0) == 0)
    def _():
        for g in range(groups):
            stack[g * 128 : (g + 1) * 128, :] = right_ref[:, g * 256 : (g + 1) * 256]

    spread_row = lax.broadcasted_iota(jnp.int32, (32, 128), 0)
    spread_col = lax.broadcasted_iota(jnp.int32, (32, 128), 1)
    spread = jnp.where(spread_col % 32 == spread_row, 1.0, 0.0).astype(BF16)
    band_row = lax.broadcasted_iota(jnp.int32, (256, 256), 0) // 64
    band_col = (lax.broadcasted_iota(jnp.int32, (256, 256), 1) % 128) // 32
    band = band_row == band_col
    outer_rows = []
    for p in range(rows // 2):
        wide = jnp.concatenate(
            [dot(left_ref[2 * p], spread), dot(left_ref[2 * p + 1], spread)], axis=1
        )
        tall = jnp.concatenate([wide] * 4, axis=0)
        weights = jnp.where(band, tall, 0.0).astype(BF16)
        outer = dot(stack[...], weights).astype(BF16)
        for k in range(2):
            outer_rows.append(
                jnp.concatenate(
                    [
                        outer[g * 128 : (g + 1) * 128, k * 128 : (k + 1) * 128]
                        for g in range(groups)
                    ],
                    axis=1,
                )
            )
    update = dot(jnp.concatenate(outer_rows, axis=0), proj_ref[...])
    pair = pair_ref[...].reshape(rows * 128, 128).astype(F32)
    fresh = (pair + update * (1.0 / 64.0) + bias_ref[...]).astype(BF16)
    new_ref[...] = fresh.reshape(rows, 128, 128)
    normed = standardize(fresh)
    normed_low = normed.astype(BF16)
    for i in range(rows):
        logit_ref[i] = dot_nt(logit_w_ref[...], normed_low[i * 128 : (i + 1) * 128])
    plane[...] = normed
    for i in range(rows):
        for q in range(4):
            turn[pl.ds(i * 4 + q, 32, stride=4 * rows), :] = plane[
                pl.ds(i * 128 + q, 32, stride=4), :
            ]
    turned_ref[...] = turn[...].reshape(32, 4 * rows, 128).astype(BF16)


def pair_stage(right, left, pair_rep, proj, bias, logit_w):
    block = 4
    steps = 32 // block
    return pl.pallas_call(
        pair_kernel,
        grid=(steps,),
        in_specs=[
            pl.BlockSpec((128, 2048), lambda b: (0, 0)),
            pl.BlockSpec((block, 64, 32), lambda b: (b, 0, 0)),
            pl.BlockSpec((block, 128, 128), lambda b: (b, 0, 0)),
            pl.BlockSpec((1024, 128), lambda b: (0, 0)),
            pl.BlockSpec((1, 128), lambda b: (0, 0)),
            pl.BlockSpec((8, 128), lambda b: (0, 0)),
        ],
        out_specs=[
            pl.BlockSpec((block, 128, 128), lambda b: (b, 0, 0)),
            pl.BlockSpec((32, 4 * block, 128), lambda b: (0, b, 0)),
            pl.BlockSpec((block, 8, 128), lambda b: (b, 0, 0)),
        ],
        out_shape=[
            jax.ShapeDtypeStruct((32, 128, 128), BF16),
            jax.ShapeDtypeStruct((32, 128, 128), BF16),
            jax.ShapeDtypeStruct((32, 8, 128), F32),
        ],
        scratch_shapes=[
            pltpu.VMEM((1024, 256), BF16),
            pltpu.VMEM((block * 128, 128), F32),
            pltpu.VMEM((block * 128, 128), F32),
        ],
        cost_estimate=cost(8_000_000_000, 6_000_000),
        name="pair_stage",
    )(right, left, pair_rep, proj, bias, logit_w)


def average_kernel(logit_ref, norm_ref, value_ref, out_ref, spare, summed, parts):
    logits = logit_ref[...].reshape(256, 128)
    peak = jnp.max(logits, axis=1, keepdims=True).astype(BF16).astype(F32)
    weights = jnp.exp(logits - peak).astype(BF16).astype(F32)
    denom = jnp.sum(weights, axis=1, keepdims=True)
    denom_high = denom.astype(BF16).astype(F32)
    lane = lax.broadcasted_iota(jnp.int32, (256, 128), 1)
    stats = jnp.where(
        lane == 0,
        denom_high,
        jnp.where(lane == 1, denom - denom_high, jnp.where(lane == 2, peak, 0.0)),
    ).astype(BF16)
    for c in range(8):
        out_ref[c, 512:544, :] = stats[c * 32 : (c + 1) * 32]
    spare[...] = weights
    by_head = jnp.concatenate(
        [spare[pl.ds(h, 32, stride=8), :] for h in range(8)], axis=0
    ).astype(BF16)
    for g in range(16):
        summed[g] = dot(by_head, norm_ref[:, g * 256 : (g + 1) * 256]).astype(BF16)
    for h in range(8):
        rows = summed[:, h * 32 : (h + 1) * 32, :].reshape(512, 256)
        parts[...] = dot(rows, value_ref[h])
        for i in range(32):
            start = h * 64 + (i % 4) * 16
            out_ref[i // 4, start : start + 16, :] = parts[
                pl.ds(i, 16, stride=32), :
            ].astype(BF16)


def average_stage(logits, norms, value):
    return pl.pallas_call(
        average_kernel,
        out_shape=jax.ShapeDtypeStruct((8, 544, 128), BF16),
        scratch_shapes=[
            pltpu.VMEM((256, 128), F32),
            pltpu.VMEM((16, 256, 256), BF16),
            pltpu.VMEM((512, 128), F32),
        ],
        cost_estimate=cost(2_000_000_000, 3_000_000),
        name="average_stage",
    )(logits, norms, value)


def combine_kernel(parts_ref, norm_ref, gate_ref, proj_ref, out_ref):
    peaks, denoms = [], []
    for p in range(8):
        stats = parts_ref[p, 512:544, :].astype(F32)
        denoms.append(stats[:, 0:1] + stats[:, 1:2])
        peaks.append(stats[:, 2:3])
    top = functools.reduce(jnp.maximum, peaks)
    scales = [jnp.exp(peak - top) for peak in peaks]
    denom = functools.reduce(jnp.add, [s * d for s, d in zip(scales, denoms)])
    factors = [jnp.broadcast_to(s / denom, (32, 128)) for s in scales]
    gate = jax.nn.sigmoid(dot(norm_ref[...], gate_ref[...]))
    gated = []
    for h in range(8):
        total = None
        for p in range(8):
            factor = jnp.concatenate(
                [
                    jnp.broadcast_to(factors[p][i * 8 + h : i * 8 + h + 1], (16, 128))
                    for i in range(4)
                ],
                axis=0,
            )
            term = parts_ref[p, h * 64 : (h + 1) * 64, :].astype(F32) * factor
            total = term if total is None else total + term
        gated.append(total * gate[:, h * 128 : (h + 1) * 128])
    wide = jnp.concatenate(gated, axis=1)
    high = wide.astype(BF16)
    rest = wide - high.astype(F32)
    middle = rest.astype(BF16)
    low = (rest - middle.astype(F32)).astype(BF16)
    proj = proj_ref[...]
    out_ref[...] = (dot(low, proj) + dot(middle, proj) + dot(high, proj)).astype(BF16)


def combine_stage(parts, norms, gate, proj):
    return pl.pallas_call(
        combine_kernel,
        out_shape=jax.ShapeDtypeStruct((64, 256), BF16),
        cost_estimate=cost(300_000_000, 2_500_000),
        name="combine_stage",
    )(parts, norms, gate, proj)


def triangle_kernel(turned_ref, proj_ref, bias_ref, inputs_ref, edge_ref, plane):
    plane[...] = turned_ref[...].reshape(512, 128).astype(F32)
    for q in range(4):
        rows = jnp.concatenate(
            [plane[pl.ds(p * 128 + q, 32, stride=4), :] for p in range(4)], axis=0
        ).astype(BF16)
        projected = dot(rows, proj_ref[...])
        inputs_ref[q, :, :384] = projected[:, :384].astype(BF16)
        inputs_ref[q, :, 384:] = jax.nn.sigmoid(projected[:, 384:]).astype(BF16)
        edge_ref[:, q, :] = dot_nt(bias_ref[...], rows)[:4].astype(BF16)


def triangle_stage(turned, proj, bias):
    return pl.pallas_call(
        triangle_kernel,
        grid=(8,),
        in_specs=[
            pl.BlockSpec((4, 128, 128), lambda b: (b, 0, 0)),
            pl.BlockSpec((128, 512), lambda b: (0, 0)),
            pl.BlockSpec((8, 128), lambda b: (0, 0)),
        ],
        out_specs=[
            pl.BlockSpec((4, 128, 512), lambda b: (0, b, 0)),
            pl.BlockSpec((4, 4, 128), lambda b: (0, 0, b)),
        ],
        out_shape=[
            jax.ShapeDtypeStruct((4, 1024, 512), BF16),
            jax.ShapeDtypeStruct((4, 4, 1024), BF16),
        ],
        scratch_shapes=[pltpu.VMEM((512, 128), F32)],
        cost_estimate=cost(1_000_000_000, 6_000_000),
        name="triangle_stage",
    )(turned, proj, bias)


def row_pairs():
    pairs = []
    for r in range(32):
        for c in range(8):
            pairs.append((r * 8 + c, (c * 4 + r // 8) * 8 + r % 8))
    return pairs


def per_device(
    alignment, pair_rep, outer_left, outer_right, outer_proj, outer_bias,
    average_value, average_gate, average_logit, average_out, triangle_proj, triangle_bias,
):
    pairs = row_pairs()
    norm = standardize(jnp.transpose(alignment, (1, 0, 2))).astype(BF16)
    right = jnp.einsum("tsm,md->tds", norm, outer_right, preferred_element_type=F32)
    left = jnp.einsum("tsm,mc->tsc", norm, outer_left, preferred_element_type=F32)
    own = jnp.concatenate(
        [right.astype(BF16).reshape(4, 2048), left.astype(BF16).reshape(4, 2048)], axis=1
    )
    norm_flat = norm.reshape(4, 4096)
    near = lax.all_gather(own, ("zh", "co"), axis=0, tiled=True)
    left_rows = lax.ppermute(near[:, 2048:], ALL, pairs)
    right_cols = lax.all_gather(near[:, :2048], "y", axis=0, tiled=True)
    norm_cols = lax.all_to_all(
        jnp.broadcast_to(norm_flat[None], (32, 4, 4096)), ROW, 0, 0, tiled=True
    ).reshape(128, 4096)
    norm_own = lax.ppermute(norm_flat, ALL, pairs)

    proj = jnp.transpose(outer_proj.reshape(32, 32, 128), (1, 0, 2)).reshape(1024, 128)
    logit_w = jnp.transpose(average_logit)
    bias_w = jnp.pad(jnp.transpose(triangle_bias), ((0, 4), (0, 0)))
    eye = jnp.eye(4, dtype=BF16)
    value_w = jnp.einsum("pq,mhc->hpmqc", eye, average_value.reshape(64, 8, 32))
    value_w = value_w.reshape(8, 256, 128)
    gate_w = jnp.einsum("pq,mhc->pmhqc", eye, average_gate.reshape(64, 8, 32))
    gate_w = gate_w.reshape(256, 1024)
    out_w = jnp.einsum("pq,hcm->hpcqm", eye, average_out.reshape(8, 32, 64))
    out_w = out_w.reshape(1024, 256)

    pair_new, turned, logits = pair_stage(
        right_cols, left_rows.reshape(32, 64, 32), pair_rep, proj,
        outer_bias.reshape(1, 128), logit_w,
    )
    turned = lax.all_to_all(turned, ROW, 0, 0, tiled=True)
    parts = average_stage(logits, norm_cols, value_w)
    parts = lax.all_to_all(parts, COL, 0, 0, tiled=True)
    update = combine_stage(parts, norm_own.reshape(64, 256), gate_w, out_w)
    alignment_update = jnp.transpose(update.reshape(4, 64, 64), (1, 0, 2))
    triangle_inputs, edge_bias = triangle_stage(turned, triangle_proj, bias_w)
    return (pair_new, alignment_update, triangle_inputs, edge_bias)


def solution(mesh):
    fine = Mesh(mesh.devices.reshape(4, 4, 2, 2, 4), ALL)
    placed = (P(None, COL + ROW, None), P(ROW, COL, None)) + (P(),) * 10
    return jax.shard_map(
        per_device,
        mesh=fine,
        in_specs=placed,
        out_specs=(
            P(ROW, COL, None),
            P(None, ROW + COL, None),
            P(COL + ROW, None, None),
            P(None, COL + ROW, None),
        ),
        check_vma=False,
    )
```

```python
import functools

import jax
import jax.numpy as jnp
from jax import lax
from jax.experimental import pallas as pl
from jax.experimental.pallas import tpu as pltpu
from jax.sharding import Mesh, PartitionSpec as P


BF16 = jnp.bfloat16
F32 = jnp.float32
ROW = ("y", "zh", "co")
COL = ("zl", "x")
ALL = ROW + COL


def dot(a, b):
    return jnp.dot(a, b, preferred_element_type=F32)


def dot_nt(a, b):
    return lax.dot_general(a, b, (((1,), (1,)), ((), ())), preferred_element_type=F32)


def cost(flops, nbytes, trans=0):
    return pl.CostEstimate(flops=flops, bytes_accessed=nbytes, transcendentals=trans)


def standardize(values):
    widened = values.astype(F32)
    centered = widened - jnp.mean(widened, axis=-1, keepdims=True)
    spread = jnp.mean(centered * centered, axis=-1, keepdims=True)
    return centered * lax.rsqrt(spread + 1e-05)


def iota(shape, dim):
    return lax.broadcasted_iota(jnp.int32, shape, dim)


def picker(rows, cols, rule):
    return jnp.where(rule(iota((rows, cols), 0), iota((rows, cols), 1)), 1.0, 0.0).astype(BF16)


def banded(wide, copies, col_period, col_width):
    tall = jnp.concatenate([wide] * copies, axis=0)
    rows, cols = tall.shape
    here = iota((rows, cols), 0) // wide.shape[0]
    there = (iota((rows, cols), 1) % col_period) // col_width
    return jnp.where(here == there, tall, 0.0).astype(BF16)


def prep_kernel(align_ref, left_ref, out_ref, wide, plane):
    wide[...] = align_ref[...].astype(F32)
    lefts = []
    for t in range(4):
        normed = standardize(wide[:, t, :]).astype(BF16)
        plane[...] = normed.astype(F32)
        out_ref[t * 32 : (t + 1) * 32, :] = jnp.concatenate(
            [plane[pl.ds(0, 32, stride=2), :], plane[pl.ds(1, 32, stride=2), :]], axis=1
        ).astype(BF16)
        lefts.append(dot(normed, left_ref[...]))
    out_ref[128:192, :] = jnp.concatenate(lefts, axis=1).astype(BF16)


def prep_stage(alignment, outer_left):
    return pl.pallas_call(
        prep_kernel,
        out_shape=jax.ShapeDtypeStruct((192, 128), BF16),
        scratch_shapes=[pltpu.VMEM((64, 4, 64), F32), pltpu.VMEM((64, 64), F32)],
        cost_estimate=cost(10_000_000, 100_000),
        name="prep_stage",
    )(alignment, outer_left)


def pair_kernel(
    norm_ref, left_ref, pair_ref, right_ref, proj_ref, bias_ref, logit_w_ref,
    new_ref, turned_ref, logit_ref, cols_ref,
    stack, proj, logit_w, wide, tall, plane, turn,
):
    rows = pair_ref.shape[0]

    @pl.when(pl.program_id(0) == 0)
    def _():
        wide[...] = norm_ref[...].astype(F32)
        spread = picker(32, 128, lambda r, c: c % 32 == r)
        right_w = banded(dot(right_ref[...], spread), 4, 128, 32)
        for g in range(16):
            cols = jnp.concatenate(
                [wide[pl.ds(2 * g + k, 128, stride=32), :] for k in range(2)], axis=1
            ).astype(BF16)
            cols_ref[:, g * 256 : (g + 1) * 256] = cols
            tall[g * 128 : (g + 1) * 128, :] = jnp.transpose(dot(cols, right_w))
        for g in range(8):
            group = jnp.concatenate(
                [tall[pl.ds(g * 4 + d, 64, stride=32), :] for d in range(4)], axis=0
            )
            stack[g * 128 : (g + 1) * 128, :] = jnp.transpose(group).astype(BF16)
        tall[0:1024, :] = proj_ref[...].astype(F32)
        for d in range(32):
            proj[d * 32 : (d + 1) * 32, :] = tall[pl.ds(d, 32, stride=32), :].astype(BF16)
        eye = picker(8, 8, lambda r, c: r == c)
        logit_w[...] = dot_nt(eye, logit_w_ref[...]).astype(BF16)

    outer_rows = []
    for p in range(rows // 2):
        choose = picker(
            128, 256, lambda r, c: (r // 32 == 2 * p + c // 128) & (r % 32 == c % 32)
        )
        weights = banded(dot(left_ref[0], choose), 4, 128, 32)
        outer = dot(stack[...], weights).astype(BF16)
        for k in range(2):
            outer_rows.append(
                jnp.concatenate(
                    [
                        outer[g * 128 : (g + 1) * 128, k * 128 : (k + 1) * 128]
                        for g in range(8)
                    ],
                    axis=1,
                )
            )
    update = dot(jnp.concatenate(outer_rows, axis=0), proj[...])
    pair = pair_ref[...].reshape(rows * 128, 128).astype(F32)
    fresh = (pair + update * (1.0 / 64.0) + bias_ref[...]).astype(BF16)
    new_ref[...] = fresh.reshape(rows, 128, 128)
    normed = standardize(fresh)
    normed_low = normed.astype(BF16)
    for i in range(rows):
        logit_ref[i] = dot_nt(logit_w[...], normed_low[i * 128 : (i + 1) * 128])
    plane[...] = normed
    for i in range(rows):
        for q in range(4):
            turn[pl.ds(i * 4 + q, 32, stride=4 * rows), :] = plane[
                pl.ds(i * 128 + q, 32, stride=4), :
            ]
    turned_ref[...] = turn[...].reshape(32, 4 * rows, 128).astype(BF16)


def pair_stage(norms, left, pair_rep, right_w, proj, bias, logit_w):
    block = 4
    steps = 32 // block
    return pl.pallas_call(
        pair_kernel,
        grid=(steps,),
        in_specs=[
            pl.BlockSpec((4096, 128), lambda b: (0, 0)),
            pl.BlockSpec((1, 64, 128), lambda b: (b, 0, 0)),
            pl.BlockSpec((block, 128, 128), lambda b: (b, 0, 0)),
            pl.BlockSpec((64, 32), lambda b: (0, 0)),
            pl.BlockSpec((1024, 128), lambda b: (0, 0)),
            pl.BlockSpec((1, 128), lambda b: (0, 0)),
            pl.BlockSpec((128, 8), lambda b: (0, 0)),
        ],
        out_specs=[
            pl.BlockSpec((block, 128, 128), lambda b: (b, 0, 0)),
            pl.BlockSpec((32, 4 * block, 128), lambda b: (0, b, 0)),
            pl.BlockSpec((block, 8, 128), lambda b: (b, 0, 0)),
            pl.BlockSpec((128, 4096), lambda b: (0, 0)),
        ],
        out_shape=[
            jax.ShapeDtypeStruct((32, 128, 128), BF16),
            jax.ShapeDtypeStruct((32, 128, 128), BF16),
            jax.ShapeDtypeStruct((32, 8, 128), F32),
            jax.ShapeDtypeStruct((128, 4096), BF16),
        ],
        scratch_shapes=[
            pltpu.VMEM((1024, 256), BF16),
            pltpu.VMEM((1024, 128), BF16),
            pltpu.VMEM((8, 128), BF16),
            pltpu.VMEM((4096, 128), F32),
            pltpu.VMEM((2048, 128), F32),
            pltpu.VMEM((block * 128, 128), F32),
            pltpu.VMEM((block * 128, 128), F32),
        ],
        cost_estimate=cost(8_000_000_000, 6_000_000),
        name="pair_stage",
    )(norms, left, pair_rep, right_w, proj, bias, logit_w)


def by_heads():
    return picker(256, 1024, lambda r, c: (r // 32 == c // 128) & (r % 32 == c % 32))


def average_kernel(me_ref, logit_ref, norm_ref, value_ref, *refs):
    outs, (spare, summed, parts) = refs[:8], refs[8:]
    me = me_ref[0]
    logits = logit_ref[...].reshape(256, 128)
    peak = jnp.max(logits, axis=1, keepdims=True).astype(BF16).astype(F32)
    weights = jnp.exp(logits - peak).astype(BF16).astype(F32)
    denom = jnp.sum(weights, axis=1, keepdims=True)
    denom_high = denom.astype(BF16).astype(F32)
    lane = iota((256, 128), 1)
    stats = jnp.where(
        lane == 0,
        denom_high,
        jnp.where(lane == 1, denom - denom_high, jnp.where(lane == 2, peak, 0.0)),
    )
    spare[...] = weights
    by_head = jnp.concatenate(
        [spare[pl.ds(h, 32, stride=8), :] for h in range(8)], axis=0
    ).astype(BF16)
    for g in range(16):
        summed[g] = dot(by_head, norm_ref[:, g * 256 : (g + 1) * 256]).astype(BF16)
    spare[...] = stats
    targets = [lax.rem(me + s, 8) for s in range(8)]
    for s in range(8):
        start = pl.multiple_of(targets[s] * 32, 32)
        outs[s][512:544, :] = spare[pl.ds(start, 32), :].astype(BF16)
    value_w = banded(dot(value_ref[...], by_heads()), 4, 128, 32)
    for h in range(8):
        rows = summed[:, h * 32 : (h + 1) * 32, :].reshape(512, 256)
        parts[...] = dot(rows, value_w[:, h * 128 : (h + 1) * 128])
        for s in range(8):
            for i in range(4):
                start = h * 64 + i * 16
                outs[s][start : start + 16, :] = parts[
                    pl.ds(targets[s] * 4 + i, 16, stride=32), :
                ].astype(BF16)


def average_stage(me, logits, norms, value):
    return pl.pallas_call(
        average_kernel,
        in_specs=[
            pl.BlockSpec(memory_space=pltpu.SMEM),
            pl.BlockSpec(memory_space=pltpu.VMEM),
            pl.BlockSpec(memory_space=pltpu.VMEM),
            pl.BlockSpec(memory_space=pltpu.VMEM),
        ],
        out_shape=[jax.ShapeDtypeStruct((544, 128), BF16)] * 8,
        scratch_shapes=[
            pltpu.VMEM((256, 128), F32),
            pltpu.VMEM((16, 256, 256), BF16),
            pltpu.VMEM((512, 128), F32),
        ],
        cost_estimate=cost(2_000_000_000, 3_000_000),
        name="average_stage",
    )(me, logits, norms, value)


def combine_kernel(*refs):
    parts, (norm_ref, gate_ref, proj_ref, out_ref, plane) = refs[:8], refs[8:]
    peaks, denoms = [], []
    for part in parts:
        stats = part[512:544, :].astype(F32)
        denoms.append(stats[:, 0:1] + stats[:, 1:2])
        peaks.append(stats[:, 2:3])
    top = functools.reduce(jnp.maximum, peaks)
    scales = [jnp.exp(peak - top) for peak in peaks]
    denom = functools.reduce(jnp.add, [s * d for s, d in zip(scales, denoms)])
    factors = [jnp.broadcast_to(s / denom, (32, 128)) for s in scales]
    plane[...] = norm_ref[...].astype(F32)
    norms = jnp.concatenate(
        [plane[pl.ds(k, 64, stride=2), :] for k in range(2)], axis=1
    ).astype(BF16)
    gate_w = banded(dot(gate_ref[...], by_heads()), 4, 128, 32)
    gate = jax.nn.sigmoid(dot(norms, gate_w))
    proj_wide = dot(proj_ref[...], picker(64, 256, lambda r, c: c % 64 == r))
    total_out = None
    for h in range(8):
        total = None
        for p in range(8):
            factor = jnp.concatenate(
                [
                    jnp.broadcast_to(factors[p][i * 8 + h : i * 8 + h + 1], (16, 128))
                    for i in range(4)
                ],
                axis=0,
            )
            term = parts[p][h * 64 : (h + 1) * 64, :].astype(F32) * factor
            total = term if total is None else total + term
        gated = total * gate[:, h * 128 : (h + 1) * 128]
        proj = banded(proj_wide[h * 32 : (h + 1) * 32, :], 4, 256, 64)
        high = gated.astype(BF16)
        rest = gated - high.astype(F32)
        middle = rest.astype(BF16)
        low = (rest - middle.astype(F32)).astype(BF16)
        term = dot(low, proj) + dot(middle, proj) + dot(high, proj)
        total_out = term if total_out is None else total_out + term
    out_ref[...] = total_out.astype(BF16)


def combine_stage(parts, norms, gate, proj):
    return pl.pallas_call(
        combine_kernel,
        out_shape=jax.ShapeDtypeStruct((64, 256), BF16),
        scratch_shapes=[pltpu.VMEM((128, 128), F32)],
        cost_estimate=cost(300_000_000, 2_500_000),
        name="combine_stage",
    )(*parts, norms, gate, proj)


def triangle_kernel(turned_ref, proj_ref, bias_ref, inputs_ref, edge_ref, plane):
    eye = picker(8, 4, lambda r, c: r == c)
    bias = dot_nt(eye, bias_ref[...]).astype(BF16)
    plane[...] = turned_ref[...].reshape(512, 128).astype(F32)
    for q in range(4):
        rows = jnp.concatenate(
            [plane[pl.ds(p * 128 + q, 32, stride=4), :] for p in range(4)], axis=0
        ).astype(BF16)
        projected = dot(rows, proj_ref[...])
        inputs_ref[q, :, :384] = projected[:, :384].astype(BF16)
        inputs_ref[q, :, 384:] = jax.nn.sigmoid(projected[:, 384:]).astype(BF16)
        edge_ref[:, q, :] = dot_nt(bias, rows)[:4].astype(BF16)


def triangle_stage(turned, proj, bias):
    return pl.pallas_call(
        triangle_kernel,
        grid=(8,),
        in_specs=[
            pl.BlockSpec((4, 128, 128), lambda b: (b, 0, 0)),
            pl.BlockSpec((128, 512), lambda b: (0, 0)),
            pl.BlockSpec((128, 4), lambda b: (0, 0)),
        ],
        out_specs=[
            pl.BlockSpec((4, 128, 512), lambda b: (0, b, 0)),
            pl.BlockSpec((4, 4, 128), lambda b: (0, 0, b)),
        ],
        out_shape=[
            jax.ShapeDtypeStruct((4, 1024, 512), BF16),
            jax.ShapeDtypeStruct((4, 4, 1024), BF16),
        ],
        scratch_shapes=[pltpu.VMEM((512, 128), F32)],
        cost_estimate=cost(1_000_000_000, 6_000_000),
        name="triangle_stage",
    )(turned, proj, bias)


def row_pairs():
    pairs = []
    for r in range(32):
        for c in range(8):
            pairs.append((r * 8 + c, (c * 4 + r // 8) * 8 + r % 8))
    return pairs


def per_device(
    alignment, pair_rep, outer_left, outer_right, outer_proj, outer_bias,
    average_value, average_gate, average_logit, average_out, triangle_proj, triangle_bias,
):
    pairs = row_pairs()
    me = (lax.axis_index("zl") * 4 + lax.axis_index("x")).astype(jnp.int32).reshape(1)
    own = prep_stage(alignment, outer_left)
    near = lax.all_gather(own, ("zh", "co"), axis=0)
    left_rows = lax.ppermute(near[:, 128:], ALL, pairs)
    norm_cols = lax.all_gather(near[:, :128], "y", axis=0).reshape(4096, 128)
    norm_own = lax.ppermute(own[:128], ALL, pairs)
    pair_new, turned, logits, cols = pair_stage(
        norm_cols, left_rows, pair_rep, outer_right, outer_proj,
        outer_bias.reshape(1, 128), average_logit,
    )
    turned = lax.all_to_all(turned, ROW, 0, 0, tiled=True)
    parts = average_stage(me, logits, cols, average_value)
    parts = [parts[0]] + [
        lax.ppermute(parts[s], COL, [(c, (c + s) % 8) for c in range(8)]) for s in range(1, 8)
    ]
    triangle_inputs, edge_bias = triangle_stage(turned, triangle_proj, triangle_bias)
    update = combine_stage(parts, norm_own, average_gate, average_out)
    alignment_update = jnp.transpose(update.reshape(4, 64, 64), (1, 0, 2))
    return (pair_new, alignment_update, triangle_inputs, edge_bias)


def solution(mesh):
    fine = Mesh(mesh.devices.reshape(4, 4, 2, 2, 4), ALL)
    placed = (P(None, COL + ROW, None), P(ROW, COL, None)) + (P(),) * 10
    return jax.shard_map(
        per_device,
        mesh=fine,
        in_specs=placed,
        out_specs=(
            P(ROW, COL, None),
            P(None, ROW + COL, None),
            P(COL + ROW, None, None),
            P(None, COL + ROW, None),
        ),
        check_vma=False,
    )
```

```python
import functools

import jax
import jax.numpy as jnp
from jax import lax
from jax.experimental import pallas as pl
from jax.experimental.pallas import tpu as pltpu
from jax.sharding import Mesh, PartitionSpec as P


BF16 = jnp.bfloat16
F32 = jnp.float32
ROW = ("y", "zh", "co")
COL = ("zl", "x")
ALL = ROW + COL


def dot(a, b):
    return jnp.dot(a, b, preferred_element_type=F32)


def dot_nt(a, b):
    return lax.dot_general(a, b, (((1,), (1,)), ((), ())), preferred_element_type=F32)


def cost(flops, nbytes, trans=0):
    return pl.CostEstimate(flops=flops, bytes_accessed=nbytes, transcendentals=trans)


def standardize(values):
    widened = values.astype(F32)
    centered = widened - jnp.mean(widened, axis=-1, keepdims=True)
    spread = jnp.mean(centered * centered, axis=-1, keepdims=True)
    return centered * lax.rsqrt(spread + 1e-05)


def iota(shape, dim):
    return lax.broadcasted_iota(jnp.int32, shape, dim)


def picker(rows, cols, rule):
    return jnp.where(rule(iota((rows, cols), 0), iota((rows, cols), 1)), 1.0, 0.0).astype(BF16)


def banded(wide, copies, col_period, col_width):
    tall = jnp.concatenate([wide] * copies, axis=0)
    rows, cols = tall.shape
    here = iota((rows, cols), 0) // wide.shape[0]
    there = (iota((rows, cols), 1) % col_period) // col_width
    return jnp.where(here == there, tall, 0.0).astype(BF16)


def prep_kernel(align_ref, left_ref, out_ref, wide, plane):
    wide[...] = align_ref[...].astype(F32)
    lefts = []
    for t in range(4):
        normed = standardize(wide[:, t, :]).astype(BF16)
        plane[...] = normed.astype(F32)
        out_ref[t * 32 : (t + 1) * 32, :] = jnp.concatenate(
            [plane[pl.ds(0, 32, stride=2), :], plane[pl.ds(1, 32, stride=2), :]], axis=1
        ).astype(BF16)
        lefts.append(dot_nt(normed, left_ref[...]))
    out_ref[128:192, :] = jnp.concatenate(lefts, axis=1).astype(BF16)


def prep_stage(alignment, outer_left):
    return pl.pallas_call(
        prep_kernel,
        out_shape=jax.ShapeDtypeStruct((192, 128), BF16),
        scratch_shapes=[pltpu.VMEM((64, 4, 64), F32), pltpu.VMEM((64, 64), F32)],
        cost_estimate=cost(10_000_000, 100_000),
        compiler_params=pltpu.CompilerParams(vmem_limit_bytes=4 * 2**20),
        name="prep_stage",
    )(alignment, outer_left)


def pair_kernel(
    norm_ref, left_ref, pair_ref, right_ref, proj_ref, bias_ref, logit_w_ref,
    new_ref, turned_ref, logit_ref, cols_ref,
    stack, proj, wide, tall, plane, turn,
):
    rows = pair_ref.shape[0]

    @pl.when(pl.program_id(0) == 0)
    def _():
        wide[...] = norm_ref[...].astype(F32)
        spread = picker(64, 256, lambda r, c: c % 64 == r)
        right_w = banded(dot(right_ref[...], spread), 4, 256, 64)
        for g in range(16):
            cols = jnp.concatenate(
                [wide[pl.ds(2 * g + k, 128, stride=32), :] for k in range(2)], axis=1
            ).astype(BF16)
            cols_ref[:, g * 256 : (g + 1) * 256] = cols
            tall[g * 128 : (g + 1) * 128, :] = dot_nt(right_w, cols)
        for g in range(8):
            group = jnp.concatenate(
                [tall[pl.ds(g * 4 + d, 64, stride=32), :] for d in range(4)], axis=0
            )
            stack[g * 128 : (g + 1) * 128, :] = jnp.transpose(group).astype(BF16)
        tall[0:1024, :] = proj_ref[...].astype(F32)
        for d in range(32):
            proj[d * 32 : (d + 1) * 32, :] = tall[pl.ds(d, 32, stride=32), :].astype(BF16)

    outer_rows = []
    for p in range(rows // 2):
        choose = picker(
            128, 256, lambda r, c: (r // 32 == 2 * p + c // 128) & (r % 32 == c % 32)
        )
        weights = banded(dot(left_ref[...], choose), 4, 128, 32)
        outer = dot(stack[...], weights).astype(BF16)
        for k in range(2):
            outer_rows.append(
                jnp.concatenate(
                    [
                        outer[g * 128 : (g + 1) * 128, k * 128 : (k + 1) * 128]
                        for g in range(8)
                    ],
                    axis=1,
                )
            )
    update = dot(jnp.concatenate(outer_rows, axis=0), proj[...])
    pair = pair_ref[...].reshape(rows * 128, 128).astype(F32)
    fresh = (pair + update * (1.0 / 64.0) + bias_ref[...]).astype(BF16)
    new_ref[...] = fresh.reshape(rows, 128, 128)
    normed = standardize(fresh)
    normed_low = normed.astype(BF16)
    for i in range(rows):
        logit_ref[i] = dot_nt(logit_w_ref[...], normed_low[i * 128 : (i + 1) * 128])
    plane[...] = normed
    for i in range(rows):
        for q in range(4):
            turn[pl.ds(i * 4 + q, 32, stride=4 * rows), :] = plane[
                pl.ds(i * 128 + q, 32, stride=4), :
            ]
    turned_ref[...] = turn[...].reshape(32, 4 * rows, 128).astype(BF16)


def pair_stage(norms, left, pair_rep, right_w, proj, bias, logit_w):
    block = 4
    steps = 32 // block
    return pl.pallas_call(
        pair_kernel,
        grid=(steps,),
        in_specs=[
            pl.BlockSpec((4096, 128), lambda b: (0, 0)),
            pl.BlockSpec((64, 128), lambda b: (b, 0)),
            pl.BlockSpec((block, 128, 128), lambda b: (b, 0, 0)),
            pl.BlockSpec((32, 64), lambda b: (0, 0)),
            pl.BlockSpec((1024, 128), lambda b: (0, 0)),
            pl.BlockSpec((1, 128), lambda b: (0, 0)),
            pl.BlockSpec((8, 128), lambda b: (0, 0)),
        ],
        out_specs=[
            pl.BlockSpec((block, 128, 128), lambda b: (b, 0, 0)),
            pl.BlockSpec((32, 4 * block, 128), lambda b: (0, b, 0)),
            pl.BlockSpec((block, 8, 128), lambda b: (b, 0, 0)),
            pl.BlockSpec((128, 4096), lambda b: (0, 0)),
        ],
        out_shape=[
            jax.ShapeDtypeStruct((32, 128, 128), BF16),
            jax.ShapeDtypeStruct((32, 128, 128), BF16),
            jax.ShapeDtypeStruct((32, 8, 128), F32),
            jax.ShapeDtypeStruct((128, 4096), BF16),
        ],
        scratch_shapes=[
            pltpu.VMEM((1024, 256), BF16),
            pltpu.VMEM((1024, 128), BF16),
            pltpu.VMEM((4096, 128), F32),
            pltpu.VMEM((2048, 128), F32),
            pltpu.VMEM((block * 128, 128), F32),
            pltpu.VMEM((block * 128, 128), F32),
        ],
        cost_estimate=cost(8_000_000_000, 6_000_000),
        compiler_params=pltpu.CompilerParams(vmem_limit_bytes=26 * 2**20),
        name="pair_stage",
    )(norms, left, pair_rep, right_w, proj, bias, logit_w)


def by_heads():
    return picker(256, 1024, lambda r, c: (r // 32 == c // 128) & (r % 32 == c % 32))


def average_kernel(me_ref, logit_ref, norm_ref, value_ref, *refs):
    outs, (spare, summed, parts) = refs[:8], refs[8:]
    me = me_ref[0]
    logits = logit_ref[...].reshape(256, 128)
    peak = jnp.max(logits, axis=1, keepdims=True).astype(BF16).astype(F32)
    weights = jnp.exp(logits - peak).astype(BF16).astype(F32)
    denom = jnp.sum(weights, axis=1, keepdims=True)
    denom_high = denom.astype(BF16).astype(F32)
    lane = iota((256, 128), 1)
    stats = jnp.where(
        lane == 0,
        denom_high,
        jnp.where(lane == 1, denom - denom_high, jnp.where(lane == 2, peak, 0.0)),
    )
    spare[...] = weights
    by_head = jnp.concatenate(
        [spare[pl.ds(h, 32, stride=8), :] for h in range(8)], axis=0
    ).astype(BF16)
    for g in range(16):
        summed[g] = dot(by_head, norm_ref[:, g * 256 : (g + 1) * 256]).astype(BF16)
    spare[...] = stats
    targets = [lax.rem(me + s, 8) for s in range(8)]
    for s in range(8):
        start = pl.multiple_of(targets[s] * 32, 32)
        outs[s][512:544, :] = spare[pl.ds(start, 32), :].astype(BF16)
    value_w = banded(dot(value_ref[...], by_heads()), 4, 128, 32)
    for h in range(8):
        rows = summed[:, h * 32 : (h + 1) * 32, :].reshape(512, 256)
        parts[...] = dot(rows, value_w[:, h * 128 : (h + 1) * 128])
        for s in range(8):
            for i in range(4):
                start = h * 64 + i * 16
                outs[s][start : start + 16, :] = parts[
                    pl.ds(targets[s] * 4 + i, 16, stride=32), :
                ].astype(BF16)


def average_stage(me, logits, norms, value):
    return pl.pallas_call(
        average_kernel,
        in_specs=[
            pl.BlockSpec(memory_space=pltpu.SMEM),
            pl.BlockSpec(memory_space=pltpu.VMEM),
            pl.BlockSpec(memory_space=pltpu.VMEM),
            pl.BlockSpec(memory_space=pltpu.VMEM),
        ],
        out_shape=[jax.ShapeDtypeStruct((544, 128), BF16)] * 8,
        scratch_shapes=[
            pltpu.VMEM((256, 128), F32),
            pltpu.VMEM((16, 256, 256), BF16),
            pltpu.VMEM((512, 128), F32),
        ],
        cost_estimate=cost(2_000_000_000, 3_000_000),
        compiler_params=pltpu.CompilerParams(vmem_limit_bytes=14 * 2**20),
        name="average_stage",
    )(me, logits, norms, value)


def combine_kernel(*refs):
    parts, (norm_ref, gate_ref, proj_ref, out_ref, plane, placed) = refs[:8], refs[8:]
    peaks, denoms = [], []
    for part in parts:
        stats = part[512:544, :].astype(F32)
        denoms.append(stats[:, 0:1] + stats[:, 1:2])
        peaks.append(stats[:, 2:3])
    top = functools.reduce(jnp.maximum, peaks)
    scales = [jnp.exp(peak - top) for peak in peaks]
    denom = functools.reduce(jnp.add, [s * d for s, d in zip(scales, denoms)])
    factors = [jnp.broadcast_to(s / denom, (32, 128)) for s in scales]
    plane[...] = norm_ref[512:640, :].astype(F32)
    norms = jnp.concatenate(
        [plane[pl.ds(k, 64, stride=2), :] for k in range(2)], axis=1
    ).astype(BF16)
    gate_w = banded(dot(gate_ref[...], by_heads()), 4, 128, 32)
    gate = jax.nn.sigmoid(dot(norms, gate_w))
    proj_w = banded(dot(proj_ref[...], by_heads()), 4, 128, 32)
    total_out = None
    for h in range(8):
        total = None
        for p in range(8):
            factor = jnp.concatenate(
                [
                    jnp.broadcast_to(factors[p][i * 8 + h : i * 8 + h + 1], (16, 128))
                    for i in range(4)
                ],
                axis=0,
            )
            term = parts[p][h * 64 : (h + 1) * 64, :].astype(F32) * factor
            total = term if total is None else total + term
        gated = total * gate[:, h * 128 : (h + 1) * 128]
        proj = proj_w[:, h * 128 : (h + 1) * 128]
        high = gated.astype(BF16)
        rest = gated - high.astype(F32)
        middle = rest.astype(BF16)
        low = (rest - middle.astype(F32)).astype(BF16)
        term = dot_nt(low, proj) + dot_nt(middle, proj) + dot_nt(high, proj)
        total_out = term if total_out is None else total_out + term
    for i in range(4):
        for k in range(4):
            placed[pl.ds(k, 16, stride=4), i, :] = total_out[
                i * 16 : (i + 1) * 16, k * 64 : (k + 1) * 64
            ]
    out_ref[...] = placed[...].astype(BF16)


def combine_stage(parts, norms, gate, proj):
    return pl.pallas_call(
        combine_kernel,
        in_specs=[pl.BlockSpec(memory_space=pltpu.VMEM)] * 11,
        out_shape=jax.ShapeDtypeStruct((64, 4, 64), BF16),
        scratch_shapes=[pltpu.VMEM((128, 128), F32), pltpu.VMEM((64, 4, 64), F32)],
        cost_estimate=cost(300_000_000, 2_500_000),
        compiler_params=pltpu.CompilerParams(vmem_limit_bytes=10 * 2**20),
        name="combine_stage",
    )(*parts, norms, gate, proj)


def triangle_kernel(turned_ref, proj_ref, bias_ref, inputs_ref, edge_ref, plane):
    start = pl.program_id(0) * 4
    plane[...] = turned_ref[pl.ds(start, 4)].reshape(512, 128).astype(F32)
    for q in range(4):
        rows = jnp.concatenate(
            [plane[pl.ds(p * 128 + q, 32, stride=4), :] for p in range(4)], axis=0
        ).astype(BF16)
        projected = dot(rows, proj_ref[...])
        inputs_ref[q, :, :384] = projected[:, :384].astype(BF16)
        inputs_ref[q, :, 384:] = jax.nn.sigmoid(projected[:, 384:]).astype(BF16)
        edge_ref[:, q, :] = dot_nt(bias_ref[...], rows).astype(BF16)


def triangle_stage(turned, proj, bias):
    return pl.pallas_call(
        triangle_kernel,
        grid=(8,),
        in_specs=[
            pl.BlockSpec(memory_space=pltpu.VMEM),
            pl.BlockSpec((128, 512), lambda b: (0, 0)),
            pl.BlockSpec((4, 128), lambda b: (0, 0)),
        ],
        out_specs=[
            pl.BlockSpec((4, 128, 512), lambda b: (0, b, 0)),
            pl.BlockSpec((4, 4, 128), lambda b: (0, 0, b)),
        ],
        out_shape=[
            jax.ShapeDtypeStruct((4, 1024, 512), BF16),
            jax.ShapeDtypeStruct((4, 4, 1024), BF16),
        ],
        scratch_shapes=[pltpu.VMEM((512, 128), F32)],
        cost_estimate=cost(1_000_000_000, 6_000_000),
        compiler_params=pltpu.CompilerParams(vmem_limit_bytes=10 * 2**20),
        name="triangle_stage",
    )(turned, proj, bias)


def row_pairs():
    pairs = []
    for r in range(32):
        for c in range(8):
            pairs.append((r * 8 + c, (c * 4 + r // 8) * 8 + r % 8))
    return pairs


def per_device(
    alignment, pair_rep, outer_left, outer_right, outer_proj, outer_bias,
    average_value, average_gate, average_logit, average_out, triangle_proj, triangle_bias,
):
    pairs = row_pairs()
    me = (lax.axis_index("zl") * 4 + lax.axis_index("x")).astype(jnp.int32).reshape(1)
    own = prep_stage(alignment, jnp.transpose(outer_left))
    near = lax.all_gather(own, ("zh", "co"), axis=0)
    rows_sent = jnp.concatenate([near[:, 128:].reshape(512, 128), own[:128]], axis=0)
    rows_here = lax.ppermute(rows_sent, ALL, pairs)
    norm_cols = lax.all_to_all(
        jnp.broadcast_to(near[None, :, :128], (4, 8, 128, 128)), "y", 0, 0, tiled=True
    ).reshape(4096, 128)
    pair_new, turned, logits, cols = pair_stage(
        norm_cols, rows_here, pair_rep, jnp.transpose(outer_right), outer_proj,
        outer_bias.reshape(1, 128), jnp.transpose(average_logit),
    )
    turned = lax.all_to_all(turned, ROW, 0, 0, tiled=True)
    parts = average_stage(me, logits, cols, average_value)
    parts = [parts[0]] + [
        lax.ppermute(parts[s], COL, [(c, (c + s) % 8) for c in range(8)]) for s in range(1, 8)
    ]
    triangle_inputs, edge_bias = triangle_stage(
        turned, triangle_proj, jnp.transpose(triangle_bias)
    )
    rows_here, edge_bias = lax.optimization_barrier((rows_here, edge_bias))
    alignment_update = combine_stage(
        parts, rows_here, average_gate, jnp.transpose(average_out)
    )
    return (pair_new, alignment_update, triangle_inputs, edge_bias)


def solution(mesh):
    fine = Mesh(mesh.devices.reshape(4, 4, 2, 2, 4), ALL)
    placed = (P(None, COL + ROW, None), P(ROW, COL, None)) + (P(),) * 10
    return jax.shard_map(
        per_device,
        mesh=fine,
        in_specs=placed,
        out_specs=(
            P(ROW, COL, None),
            P(None, ROW + COL, None),
            P(COL + ROW, None, None),
            P(None, COL + ROW, None),
        ),
        check_vma=False,
    )
```

```python
import functools

import jax
import jax.numpy as jnp
from jax import lax
from jax.experimental import pallas as pl
from jax.experimental.pallas import tpu as pltpu
from jax.sharding import Mesh, PartitionSpec as P


BF16 = jnp.bfloat16
F32 = jnp.float32
ROW = ("y", "zh", "co")
COL = ("zl", "x")
ALL = ROW + COL


def dot(a, b):
    return jnp.dot(a, b, preferred_element_type=F32)


def dot_nt(a, b):
    return lax.dot_general(a, b, (((1,), (1,)), ((), ())), preferred_element_type=F32)


def cost(flops, nbytes, trans=0):
    return pl.CostEstimate(flops=flops, bytes_accessed=nbytes, transcendentals=trans)


def standardize(values):
    widened = values.astype(F32)
    centered = widened - jnp.mean(widened, axis=-1, keepdims=True)
    spread = jnp.mean(centered * centered, axis=-1, keepdims=True)
    return centered * lax.rsqrt(spread + 1e-05)


def iota(shape, dim):
    return lax.broadcasted_iota(jnp.int32, shape, dim)


def picker(rows, cols, rule):
    return jnp.where(rule(iota((rows, cols), 0), iota((rows, cols), 1)), 1.0, 0.0).astype(BF16)


def banded(wide, copies, col_period, col_width):
    tall = jnp.concatenate([wide] * copies, axis=0)
    rows, cols = tall.shape
    here = iota((rows, cols), 0) // wide.shape[0]
    there = (iota((rows, cols), 1) % col_period) // col_width
    return jnp.where(here == there, tall, 0.0).astype(BF16)


def prep_kernel(align_ref, left_ref, out_ref, wide, plane):
    wide[...] = align_ref[...].astype(F32)
    lefts = []
    for t in range(4):
        normed = standardize(wide[:, t, :]).astype(BF16)
        plane[...] = normed.astype(F32)
        out_ref[t * 32 : (t + 1) * 32, :] = jnp.concatenate(
            [plane[pl.ds(0, 32, stride=2), :], plane[pl.ds(1, 32, stride=2), :]], axis=1
        ).astype(BF16)
        lefts.append(dot_nt(normed, left_ref[...]))
    out_ref[128:192, :] = jnp.concatenate(lefts, axis=1).astype(BF16)


def prep_stage(alignment, outer_left):
    return pl.pallas_call(
        prep_kernel,
        out_shape=jax.ShapeDtypeStruct((192, 128), BF16),
        scratch_shapes=[pltpu.VMEM((64, 4, 64), F32), pltpu.VMEM((64, 64), F32)],
        cost_estimate=cost(10_000_000, 100_000),
        compiler_params=pltpu.CompilerParams(vmem_limit_bytes=4 * 2**20),
        name="prep_stage",
    )(alignment, outer_left)


def right_kernel(norm_ref, right_ref, out_ref, wide, tall):
    wide[...] = norm_ref[...].reshape(1024, 128).astype(F32)
    rows = dot(picker(256, 32, lambda r, c: r // 8 == c), right_ref[...]).astype(BF16)
    rows = dot(rows, picker(64, 512, lambda r, c: c % 64 == r))
    here = iota((256, 512), 0) % 8
    there = iota((256, 512), 1) // 64
    weights = jnp.where(here == there, rows, 0.0).astype(BF16)
    for g in range(8):
        cols = jnp.concatenate(
            [wide[pl.ds(4 * g + k, 32, stride=32), :] for k in range(4)], axis=1
        ).astype(BF16)
        tall[g] = dot_nt(weights, cols)
    for g in range(8):
        group = jnp.concatenate(
            [
                tall[k, (g * 4 + d) * 8 : (g * 4 + d + 1) * 8, :]
                for d in range(4)
                for k in range(8)
            ],
            axis=0,
        )
        out_ref[g] = jnp.transpose(group).astype(BF16)


def right_stage(norms, right_w):
    return pl.pallas_call(
        right_kernel,
        out_shape=jax.ShapeDtypeStruct((8, 32, 256), BF16),
        scratch_shapes=[pltpu.VMEM((1024, 128), F32), pltpu.VMEM((8, 256, 32), F32)],
        cost_estimate=cost(500_000_000, 500_000),
        compiler_params=pltpu.CompilerParams(vmem_limit_bytes=8 * 2**20),
        name="right_stage",
    )(norms, right_w)


def pair_kernel(
    right_ref, left_ref, pair_ref, proj_ref, bias_ref, logit_w_ref,
    new_ref, turned_ref, logit_ref,
    stack, proj, tall, plane, turn,
):
    rows = pair_ref.shape[0]

    @pl.when(pl.program_id(0) == 0)
    def _():
        for g in range(8):
            for y in range(4):
                start = g * 128 + y * 32
                stack[start : start + 32, :] = right_ref[y, g]
        tall[...] = proj_ref[...].astype(F32)
        for d in range(32):
            proj[d * 32 : (d + 1) * 32, :] = tall[pl.ds(d, 32, stride=32), :].astype(BF16)

    for quad in range(rows // 4):
        outer_rows = []
        for p in range(2):
            choose = picker(
                128, 256, lambda r, c: (r // 32 == 2 * p + c // 128) & (r % 32 == c % 32)
            )
            wide = dot(left_ref[quad * 64 : (quad + 1) * 64, :], choose)
            outer = dot(stack[...], banded(wide, 4, 128, 32)).astype(BF16)
            for k in range(2):
                outer_rows.append(
                    jnp.concatenate(
                        [
                            outer[g * 128 : (g + 1) * 128, k * 128 : (k + 1) * 128]
                            for g in range(8)
                        ],
                        axis=1,
                    )
                )
        update = dot(jnp.concatenate(outer_rows, axis=0), proj[...])
        four = slice(quad * 4, (quad + 1) * 4)
        pair = pair_ref[four].reshape(512, 128).astype(F32)
        fresh = (pair + update * (1.0 / 64.0) + bias_ref[...]).astype(BF16)
        new_ref[four] = fresh.reshape(4, 128, 128)
        normed = standardize(fresh)
        normed_low = normed.astype(BF16)
        for i in range(4):
            logit_ref[quad * 4 + i] = dot_nt(
                logit_w_ref[...], normed_low[i * 128 : (i + 1) * 128]
            )
        plane[quad] = normed
        for i in range(4):
            for q in range(4):
                turn[pl.ds((quad * 4 + i) * 4 + q, 32, stride=4 * rows), :] = plane[
                    quad, pl.ds(i * 128 + q, 32, stride=4), :
                ]
    turned_ref[...] = turn[...].reshape(32, 4 * rows, 128).astype(BF16)


def pair_stage(right, left, pair_rep, proj, bias, logit_w):
    block = 8
    steps = 32 // block
    return pl.pallas_call(
        pair_kernel,
        grid=(steps,),
        in_specs=[
            pl.BlockSpec((4, 8, 32, 256), lambda b: (0, 0, 0, 0)),
            pl.BlockSpec((16 * block, 128), lambda b: (b, 0)),
            pl.BlockSpec((block, 128, 128), lambda b: (b, 0, 0)),
            pl.BlockSpec((1024, 128), lambda b: (0, 0)),
            pl.BlockSpec((1, 128), lambda b: (0, 0)),
            pl.BlockSpec((8, 128), lambda b: (0, 0)),
        ],
        out_specs=[
            pl.BlockSpec((block, 128, 128), lambda b: (b, 0, 0)),
            pl.BlockSpec((32, 4 * block, 128), lambda b: (0, b, 0)),
            pl.BlockSpec((block, 8, 128), lambda b: (b, 0, 0)),
        ],
        out_shape=[
            jax.ShapeDtypeStruct((32, 128, 128), BF16),
            jax.ShapeDtypeStruct((32, 128, 128), BF16),
            jax.ShapeDtypeStruct((32, 8, 128), F32),
        ],
        scratch_shapes=[
            pltpu.VMEM((1024, 256), BF16),
            pltpu.VMEM((1024, 128), BF16),
            pltpu.VMEM((1024, 128), F32),
            pltpu.VMEM((block // 4, 512, 128), F32),
            pltpu.VMEM((block * 128, 128), F32),
        ],
        cost_estimate=cost(8_000_000_000, 6_000_000),
        compiler_params=pltpu.CompilerParams(vmem_limit_bytes=26 * 2**20),
        name="pair_stage",
    )(right, left, pair_rep, proj, bias, logit_w)


def by_heads():
    return picker(256, 1024, lambda r, c: (r // 32 == c // 128) & (r % 32 == c % 32))


def pack_stats(denom, peak):
    high = denom.astype(BF16).astype(F32)
    lane = iota((denom.shape[0], 128), 1)
    return jnp.where(
        lane == 0,
        high,
        jnp.where(lane == 1, denom - high, jnp.where(lane == 2, peak, 0.0)),
    )


def average_kernel(me_ref, logit_ref, norm_ref, value_ref, *refs):
    outs, (wide, spare, summed, parts) = refs[:4], refs[4:]
    me_z, me_x = me_ref[0], me_ref[1]
    logits = logit_ref[...].reshape(256, 128)
    peak = jnp.max(logits, axis=1, keepdims=True).astype(BF16).astype(F32)
    weights = jnp.exp(logits - peak).astype(BF16).astype(F32)
    stats = pack_stats(jnp.sum(weights, axis=1, keepdims=True), peak)
    spare[...] = weights
    by_head = jnp.concatenate(
        [spare[pl.ds(h, 32, stride=8), :] for h in range(8)], axis=0
    ).astype(BF16)
    wide[...] = norm_ref[...].astype(F32)
    for g in range(16):
        cols = jnp.concatenate(
            [wide[pl.ds(2 * g + k, 128, stride=32), :] for k in range(2)], axis=1
        ).astype(BF16)
        summed[g] = dot(by_head, cols).astype(BF16)
    spare[...] = stats
    targets = [
        [lax.rem(me_z + k, 2) * 4 + lax.rem(me_x + s, 4) for k in range(2)] for s in range(4)
    ]
    for s in range(4):
        for k in range(2):
            start = pl.multiple_of(targets[s][k] * 32, 32)
            outs[s][k, 512:544, :] = spare[pl.ds(start, 32), :].astype(BF16)
    value_w = banded(dot(value_ref[...], by_heads()), 4, 128, 32)
    for h in range(8):
        rows = summed[:, h * 32 : (h + 1) * 32, :].reshape(512, 256)
        parts[...] = dot(rows, value_w[:, h * 128 : (h + 1) * 128])
        for s in range(4):
            for k in range(2):
                for i in range(4):
                    start = h * 64 + i * 16
                    outs[s][k, start : start + 16, :] = parts[
                        pl.ds(targets[s][k] * 4 + i, 16, stride=32), :
                    ].astype(BF16)


def average_stage(me, logits, norms, value):
    return pl.pallas_call(
        average_kernel,
        in_specs=[
            pl.BlockSpec(memory_space=pltpu.SMEM),
            pl.BlockSpec(memory_space=pltpu.VMEM),
            pl.BlockSpec(memory_space=pltpu.VMEM),
            pl.BlockSpec(memory_space=pltpu.VMEM),
        ],
        out_shape=[jax.ShapeDtypeStruct((2, 544, 128), BF16)] * 4,
        scratch_shapes=[
            pltpu.VMEM((4096, 128), F32),
            pltpu.VMEM((256, 128), F32),
            pltpu.VMEM((16, 256, 256), BF16),
            pltpu.VMEM((512, 128), F32),
        ],
        cost_estimate=cost(2_000_000_000, 3_000_000),
        compiler_params=pltpu.CompilerParams(vmem_limit_bytes=16 * 2**20),
        name="average_stage",
    )(me, logits, norms, value)


def merge_stats(stats):
    denoms = [st[:, 0:1] + st[:, 1:2] for st in stats]
    peaks = [st[:, 2:3] for st in stats]
    top = functools.reduce(jnp.maximum, peaks)
    scales = [jnp.exp(peak - top) for peak in peaks]
    denom = functools.reduce(jnp.add, [s * d for s, d in zip(scales, denoms)])
    return top, scales, denom


def head_rows(factor, h):
    return jnp.concatenate(
        [jnp.broadcast_to(factor[i * 8 + h : i * 8 + h + 1], (16, 128)) for i in range(4)],
        axis=0,
    )


def merge_kernel(a_ref, b_ref, c_ref, d_ref, keep_ref, send_ref):
    sources = (a_ref, b_ref, c_ref, d_ref)
    for k, out in ((1, send_ref), (0, keep_ref)):
        top, scales, denom = merge_stats([r[k, 512:544, :].astype(F32) for r in sources])
        out[512:544, :] = pack_stats(denom, top).astype(out.dtype)
        factors = [jnp.broadcast_to(s, (32, 128)) for s in scales]
        for h in range(8):
            span = slice(h * 64, (h + 1) * 64)
            terms = [
                r[k, span, :].astype(F32) * head_rows(f, h) for r, f in zip(sources, factors)
            ]
            out[span, :] = ((terms[0] + terms[1]) + (terms[2] + terms[3])).astype(out.dtype)


def merge_stage(parts):
    return pl.pallas_call(
        merge_kernel,
        in_specs=[pl.BlockSpec(memory_space=pltpu.VMEM)] * 4,
        out_shape=[
            jax.ShapeDtypeStruct((544, 128), F32),
            jax.ShapeDtypeStruct((544, 128), BF16),
        ],
        cost_estimate=cost(10_000_000, 2_000_000),
        compiler_params=pltpu.CompilerParams(vmem_limit_bytes=6 * 2**20),
        name="merge_stage",
    )(*parts)


def combine_kernel(
    kept_ref, got_ref, norm_ref, gate_ref, proj_ref, out_ref, plane, placed
):
    parts = (kept_ref, got_ref)
    _, scales, denom = merge_stats([r[512:544, :].astype(F32) for r in parts])
    factors = [jnp.broadcast_to(s / denom, (32, 128)) for s in scales]
    plane[...] = norm_ref[512:640, :].astype(F32)
    norms = jnp.concatenate(
        [plane[pl.ds(k, 64, stride=2), :] for k in range(2)], axis=1
    ).astype(BF16)
    gate_w = banded(dot(gate_ref[...], by_heads()), 4, 128, 32)
    gate = jax.nn.sigmoid(dot(norms, gate_w))
    proj_w = banded(dot(proj_ref[...], by_heads()), 4, 128, 32)
    total_out = None
    for h in range(8):
        span = slice(h * 64, (h + 1) * 64)
        total = functools.reduce(
            jnp.add,
            [r[span, :].astype(F32) * head_rows(f, h) for r, f in zip(parts, factors)],
        )
        gated = total * gate[:, h * 128 : (h + 1) * 128]
        proj = proj_w[:, h * 128 : (h + 1) * 128]
        high = gated.astype(BF16)
        rest = gated - high.astype(F32)
        middle = rest.astype(BF16)
        low = (rest - middle.astype(F32)).astype(BF16)
        term = dot_nt(low, proj) + dot_nt(middle, proj) + dot_nt(high, proj)
        total_out = term if total_out is None else total_out + term
    for i in range(4):
        for k in range(4):
            placed[pl.ds(k, 16, stride=4), i, :] = total_out[
                i * 16 : (i + 1) * 16, k * 64 : (k + 1) * 64
            ]
    out_ref[...] = placed[...].astype(BF16)


def combine_stage(kept, got, norms, gate, proj):
    return pl.pallas_call(
        combine_kernel,
        in_specs=[pl.BlockSpec(memory_space=pltpu.VMEM)] * 5,
        out_shape=jax.ShapeDtypeStruct((64, 4, 64), BF16),
        scratch_shapes=[pltpu.VMEM((128, 128), F32), pltpu.VMEM((64, 4, 64), F32)],
        cost_estimate=cost(300_000_000, 2_500_000),
        compiler_params=pltpu.CompilerParams(vmem_limit_bytes=10 * 2**20),
        name="combine_stage",
    )(kept, got, norms, gate, proj)


def triangle_kernel(turned_ref, proj_ref, bias_ref, inputs_ref, edge_ref, plane):
    start = pl.program_id(0) * 4
    plane[...] = turned_ref[pl.ds(start, 4)].reshape(512, 128).astype(F32)
    for q in range(4):
        rows = jnp.concatenate(
            [plane[pl.ds(p * 128 + q, 32, stride=4), :] for p in range(4)], axis=0
        ).astype(BF16)
        projected = dot(rows, proj_ref[...])
        inputs_ref[q, :, :384] = projected[:, :384].astype(BF16)
        inputs_ref[q, :, 384:] = jax.nn.sigmoid(projected[:, 384:]).astype(BF16)
        edge_ref[:, q, :] = dot_nt(bias_ref[...], rows).astype(BF16)


def triangle_stage(turned, proj, bias):
    return pl.pallas_call(
        triangle_kernel,
        grid=(8,),
        in_specs=[
            pl.BlockSpec(memory_space=pltpu.VMEM),
            pl.BlockSpec((128, 512), lambda b: (0, 0)),
            pl.BlockSpec((4, 128), lambda b: (0, 0)),
        ],
        out_specs=[
            pl.BlockSpec((4, 128, 512), lambda b: (0, b, 0)),
            pl.BlockSpec((4, 4, 128), lambda b: (0, 0, b)),
        ],
        out_shape=[
            jax.ShapeDtypeStruct((4, 1024, 512), BF16),
            jax.ShapeDtypeStruct((4, 4, 1024), BF16),
        ],
        scratch_shapes=[pltpu.VMEM((512, 128), F32)],
        cost_estimate=cost(1_000_000_000, 6_000_000),
        compiler_params=pltpu.CompilerParams(vmem_limit_bytes=10 * 2**20),
        name="triangle_stage",
    )(turned, proj, bias)


def row_pairs():
    pairs = []
    for r in range(32):
        for c in range(8):
            pairs.append((r * 8 + c, (c * 4 + r // 8) * 8 + r % 8))
    return pairs


def per_device(
    alignment, pair_rep, outer_left, outer_right, outer_proj, outer_bias,
    average_value, average_gate, average_logit, average_out, triangle_proj, triangle_bias,
):
    pairs = row_pairs()
    me = jnp.stack([lax.axis_index("zl"), lax.axis_index("x")]).astype(jnp.int32)
    own = prep_stage(alignment, jnp.transpose(outer_left))
    near = lax.all_gather(own, ("zh", "co"), axis=0)
    rows_sent = jnp.concatenate([near[:, 128:].reshape(512, 128), own[:128]], axis=0)
    rows_here = lax.ppermute(rows_sent, ALL, pairs)
    near_norm = near[:, :128]
    right = right_stage(near_norm, jnp.transpose(outer_right))
    right = lax.all_to_all(
        jnp.broadcast_to(right[None], (4, 8, 32, 256)), "y", 0, 0, tiled=True
    )
    near_norm, right = lax.optimization_barrier((near_norm, right))
    norm_cols = lax.all_to_all(
        jnp.broadcast_to(near_norm[None], (4, 8, 128, 128)), "y", 0, 0, tiled=True
    ).reshape(4096, 128)
    pair_new, turned, logits = pair_stage(
        right, rows_here, pair_rep, outer_proj,
        outer_bias.reshape(1, 128), jnp.transpose(average_logit),
    )
    turned = lax.all_to_all(turned, ROW, 0, 0, tiled=True)
    parts = average_stage(me, logits, norm_cols, average_value)
    parts = [parts[0]] + [
        lax.ppermute(parts[s], "x", [(c, (c + s) % 4) for c in range(4)]) for s in range(1, 4)
    ]
    kept, sent = merge_stage(parts)
    got = lax.ppermute(sent, "zl", [(0, 1), (1, 0)])
    turned, kept = lax.optimization_barrier((turned, kept))
    triangle_inputs, edge_bias = triangle_stage(
        turned, triangle_proj, jnp.transpose(triangle_bias)
    )
    rows_here, edge_bias = lax.optimization_barrier((rows_here, edge_bias))
    alignment_update = combine_stage(
        kept, got, rows_here, average_gate, jnp.transpose(average_out)
    )
    return (pair_new, alignment_update, triangle_inputs, edge_bias)


def solution(mesh):
    fine = Mesh(mesh.devices.reshape(4, 4, 2, 2, 4), ALL)
    placed = (P(None, COL + ROW, None), P(ROW, COL, None)) + (P(),) * 10
    return jax.shard_map(
        per_device,
        mesh=fine,
        in_specs=placed,
        out_specs=(
            P(ROW, COL, None),
            P(None, ROW + COL, None),
            P(COL + ROW, None, None),
            P(None, COL + ROW, None),
        ),
        check_vma=False,
    )
```

```python
import functools

import jax
import jax.numpy as jnp
from jax import lax
from jax.experimental import pallas as pl
from jax.experimental.pallas import tpu as pltpu
from jax.sharding import Mesh, PartitionSpec as P


BF16 = jnp.bfloat16
F32 = jnp.float32
ROW = ("y", "zh", "co")
COL = ("zl", "x")
ALL = ROW + COL


def dot(a, b):
    return jnp.dot(a, b, preferred_element_type=F32)


def dot_nt(a, b):
    return lax.dot_general(a, b, (((1,), (1,)), ((), ())), preferred_element_type=F32)


def cost(flops, nbytes, trans=0):
    return pl.CostEstimate(flops=flops, bytes_accessed=nbytes, transcendentals=trans)


def standardize(values):
    widened = values.astype(F32)
    centered = widened - jnp.mean(widened, axis=-1, keepdims=True)
    spread = jnp.mean(centered * centered, axis=-1, keepdims=True)
    return centered * lax.rsqrt(spread + 1e-05)


def iota(shape, dim):
    return lax.broadcasted_iota(jnp.int32, shape, dim)


def picker(rows, cols, rule):
    return jnp.where(rule(iota((rows, cols), 0), iota((rows, cols), 1)), 1.0, 0.0).astype(BF16)


def banded(wide, copies, col_period, col_width):
    tall = jnp.concatenate([wide] * copies, axis=0)
    rows, cols = tall.shape
    here = iota((rows, cols), 0) // wide.shape[0]
    there = (iota((rows, cols), 1) % col_period) // col_width
    return jnp.where(here == there, tall, 0.0).astype(BF16)


def prep_kernel(align_ref, left_ref, out_ref, wide, plane):
    wide[...] = align_ref[...].astype(F32)
    lefts = []
    for t in range(4):
        normed = standardize(wide[:, t, :]).astype(BF16)
        plane[...] = normed.astype(F32)
        out_ref[t * 32 : (t + 1) * 32, :] = jnp.concatenate(
            [plane[pl.ds(0, 32, stride=2), :], plane[pl.ds(1, 32, stride=2), :]], axis=1
        ).astype(BF16)
        lefts.append(dot_nt(normed, left_ref[...]))
    out_ref[128:192, :] = jnp.concatenate(lefts, axis=1).astype(BF16)


def prep_stage(alignment, outer_left):
    return pl.pallas_call(
        prep_kernel,
        out_shape=jax.ShapeDtypeStruct((192, 128), BF16),
        scratch_shapes=[pltpu.VMEM((64, 4, 64), F32), pltpu.VMEM((64, 64), F32)],
        cost_estimate=cost(10_000_000, 100_000),
        compiler_params=pltpu.CompilerParams(vmem_limit_bytes=4 * 2**20),
        name="prep_stage",
    )(alignment, outer_left)


def right_kernel(near_ref, right_ref, out_ref, norm_ref, wide, tall):
    norms = near_ref[:, :128, :]
    norm_ref[...] = norms
    wide[...] = norms.reshape(1024, 128).astype(F32)
    rows = dot(picker(256, 32, lambda r, c: r // 8 == c), right_ref[...]).astype(BF16)
    rows = dot(rows, picker(64, 512, lambda r, c: c % 64 == r))
    here = iota((256, 512), 0) % 8
    there = iota((256, 512), 1) // 64
    weights = jnp.where(here == there, rows, 0.0).astype(BF16)
    for g in range(8):
        cols = jnp.concatenate(
            [wide[pl.ds(4 * g + k, 32, stride=32), :] for k in range(4)], axis=1
        ).astype(BF16)
        tall[g] = dot_nt(weights, cols)
    for g in range(8):
        group = jnp.concatenate(
            [
                tall[k, (g * 4 + d) * 8 : (g * 4 + d + 1) * 8, :]
                for d in range(4)
                for k in range(8)
            ],
            axis=0,
        )
        out_ref[g] = jnp.transpose(group).astype(BF16)


def right_stage(near, right_w):
    return pl.pallas_call(
        right_kernel,
        in_specs=[pl.BlockSpec(memory_space=pltpu.VMEM)] * 2,
        out_shape=[
            jax.ShapeDtypeStruct((8, 32, 256), BF16),
            jax.ShapeDtypeStruct((8, 128, 128), BF16),
        ],
        scratch_shapes=[pltpu.VMEM((1024, 128), F32), pltpu.VMEM((8, 256, 32), F32)],
        cost_estimate=cost(500_000_000, 500_000),
        compiler_params=pltpu.CompilerParams(vmem_limit_bytes=8 * 2**20),
        name="right_stage",
    )(near, right_w)


def pair_kernel(
    right_ref, left_ref, pair_ref, proj_ref, bias_ref, logit_w_ref,
    new_ref, turned_ref, logit_ref,
    stack, proj, tall, plane, turn,
):
    rows = pair_ref.shape[0]

    @pl.when(pl.program_id(0) == 0)
    def _():
        for g in range(8):
            for y in range(4):
                start = g * 128 + y * 32
                stack[start : start + 32, :] = right_ref[y, g]
        tall[...] = proj_ref[...].astype(F32)
        for d in range(32):
            proj[d * 32 : (d + 1) * 32, :] = tall[pl.ds(d, 32, stride=32), :].astype(BF16)

    for quad in range(rows // 4):
        outer_rows = []
        for p in range(2):
            choose = picker(
                128, 256, lambda r, c: (r // 32 == 2 * p + c // 128) & (r % 32 == c % 32)
            )
            wide = dot(left_ref[quad * 64 : (quad + 1) * 64, :], choose)
            outer = dot(stack[...], banded(wide, 4, 128, 32)).astype(BF16)
            for k in range(2):
                outer_rows.append(
                    jnp.concatenate(
                        [
                            outer[g * 128 : (g + 1) * 128, k * 128 : (k + 1) * 128]
                            for g in range(8)
                        ],
                        axis=1,
                    )
                )
        update = dot(jnp.concatenate(outer_rows, axis=0), proj[...])
        four = slice(quad * 4, (quad + 1) * 4)
        pair = pair_ref[four].reshape(512, 128).astype(F32)
        fresh = (pair + update * (1.0 / 64.0) + bias_ref[...]).astype(BF16)
        new_ref[four] = fresh.reshape(4, 128, 128)
        normed = standardize(fresh)
        normed_low = normed.astype(BF16)
        for i in range(4):
            logit_ref[quad * 4 + i] = dot_nt(
                logit_w_ref[...], normed_low[i * 128 : (i + 1) * 128]
            )
        plane[quad] = normed
        for i in range(4):
            for q in range(4):
                turn[pl.ds((quad * 4 + i) * 4 + q, 32, stride=4 * rows), :] = plane[
                    quad, pl.ds(i * 128 + q, 32, stride=4), :
                ]
    turned_ref[...] = turn[...].reshape(32, 4 * rows, 128).astype(BF16)


def pair_stage(right, left, pair_rep, proj, bias, logit_w):
    block = 8
    steps = 32 // block
    return pl.pallas_call(
        pair_kernel,
        grid=(steps,),
        in_specs=[
            pl.BlockSpec((4, 8, 32, 256), lambda b: (0, 0, 0, 0)),
            pl.BlockSpec((16 * block, 128), lambda b: (b, 0)),
            pl.BlockSpec((block, 128, 128), lambda b: (b, 0, 0)),
            pl.BlockSpec((1024, 128), lambda b: (0, 0)),
            pl.BlockSpec((1, 128), lambda b: (0, 0)),
            pl.BlockSpec((8, 128), lambda b: (0, 0)),
        ],
        out_specs=[
            pl.BlockSpec((block, 128, 128), lambda b: (b, 0, 0)),
            pl.BlockSpec((32, 4 * block, 128), lambda b: (0, b, 0)),
            pl.BlockSpec((block, 8, 128), lambda b: (b, 0, 0)),
        ],
        out_shape=[
            jax.ShapeDtypeStruct((32, 128, 128), BF16),
            jax.ShapeDtypeStruct((32, 128, 128), BF16),
            jax.ShapeDtypeStruct((32, 8, 128), F32),
        ],
        scratch_shapes=[
            pltpu.VMEM((1024, 256), BF16),
            pltpu.VMEM((1024, 128), BF16),
            pltpu.VMEM((1024, 128), F32),
            pltpu.VMEM((block // 4, 512, 128), F32),
            pltpu.VMEM((block * 128, 128), F32),
        ],
        cost_estimate=cost(8_000_000_000, 6_000_000),
        compiler_params=pltpu.CompilerParams(vmem_limit_bytes=26 * 2**20),
        name="pair_stage",
    )(right, left, pair_rep, proj, bias, logit_w)


def by_heads():
    return picker(256, 1024, lambda r, c: (r // 32 == c // 128) & (r % 32 == c % 32))


def pack_stats(denom, peak):
    high = denom.astype(BF16).astype(F32)
    lane = iota((denom.shape[0], 128), 1)
    return jnp.where(
        lane == 0,
        high,
        jnp.where(lane == 1, denom - high, jnp.where(lane == 2, peak, 0.0)),
    )


def average_kernel(me_ref, logit_ref, value_ref, *refs):
    norms, outs, (wide, spare, summed, parts) = refs[:4], refs[4:8], refs[8:]
    me_y, me_z, me_x = me_ref[0], me_ref[1], me_ref[2]
    logits = logit_ref[...].reshape(256, 128)
    peak = jnp.max(logits, axis=1, keepdims=True).astype(BF16).astype(F32)
    weights = jnp.exp(logits - peak).astype(BF16).astype(F32)
    stats = pack_stats(jnp.sum(weights, axis=1, keepdims=True), peak)
    spare[...] = weights
    by_head = jnp.concatenate(
        [spare[pl.ds(h, 32, stride=8), :] for h in range(8)], axis=0
    ).astype(BF16)
    for s in range(4):
        start = pl.multiple_of(lax.rem(me_y + 4 - s, 4) * 1024, 1024)
        wide[pl.ds(start, 1024), :] = norms[s][...].reshape(1024, 128).astype(F32)
    for g in range(16):
        cols = jnp.concatenate(
            [wide[pl.ds(2 * g + k, 128, stride=32), :] for k in range(2)], axis=1
        ).astype(BF16)
        summed[g] = dot(by_head, cols).astype(BF16)
    spare[...] = stats
    targets = [
        [lax.rem(me_z + k, 2) * 4 + lax.rem(me_x + s, 4) for k in range(2)] for s in range(4)
    ]
    for s in range(4):
        for k in range(2):
            start = pl.multiple_of(targets[s][k] * 32, 32)
            outs[s][k, 512:544, :] = spare[pl.ds(start, 32), :].astype(BF16)
    value_w = banded(dot(value_ref[...], by_heads()), 4, 128, 32)
    for h in range(8):
        rows = summed[:, h * 32 : (h + 1) * 32, :].reshape(512, 256)
        parts[...] = dot(rows, value_w[:, h * 128 : (h + 1) * 128])
        for s in range(4):
            for k in range(2):
                for i in range(4):
                    start = h * 64 + i * 16
                    outs[s][k, start : start + 16, :] = parts[
                        pl.ds(targets[s][k] * 4 + i, 16, stride=32), :
                    ].astype(BF16)


def average_stage(me, logits, value, norms):
    return pl.pallas_call(
        average_kernel,
        in_specs=[
            pl.BlockSpec(memory_space=pltpu.SMEM),
        ]
        + [pl.BlockSpec(memory_space=pltpu.VMEM)] * 6,
        out_shape=[jax.ShapeDtypeStruct((2, 544, 128), BF16)] * 4,
        scratch_shapes=[
            pltpu.VMEM((4096, 128), F32),
            pltpu.VMEM((256, 128), F32),
            pltpu.VMEM((16, 256, 256), BF16),
            pltpu.VMEM((512, 128), F32),
        ],
        cost_estimate=cost(2_000_000_000, 3_000_000),
        compiler_params=pltpu.CompilerParams(vmem_limit_bytes=16 * 2**20),
        name="average_stage",
    )(me, logits, value, *norms)


def merge_stats(stats):
    denoms = [st[:, 0:1] + st[:, 1:2] for st in stats]
    peaks = [st[:, 2:3] for st in stats]
    top = functools.reduce(jnp.maximum, peaks)
    scales = [jnp.exp(peak - top) for peak in peaks]
    denom = functools.reduce(jnp.add, [s * d for s, d in zip(scales, denoms)])
    return top, scales, denom


def head_rows(factor, h):
    return jnp.concatenate(
        [jnp.broadcast_to(factor[i * 8 + h : i * 8 + h + 1], (16, 128)) for i in range(4)],
        axis=0,
    )


def merge_kernel(a_ref, b_ref, c_ref, d_ref, keep_ref, send_ref):
    sources = (a_ref, b_ref, c_ref, d_ref)
    for k, out in ((1, send_ref), (0, keep_ref)):
        top, scales, denom = merge_stats([r[k, 512:544, :].astype(F32) for r in sources])
        out[512:544, :] = pack_stats(denom, top).astype(out.dtype)
        factors = [jnp.broadcast_to(s, (32, 128)) for s in scales]
        for h in range(8):
            span = slice(h * 64, (h + 1) * 64)
            terms = [
                r[k, span, :].astype(F32) * head_rows(f, h) for r, f in zip(sources, factors)
            ]
            out[span, :] = ((terms[0] + terms[1]) + (terms[2] + terms[3])).astype(out.dtype)


def merge_stage(parts):
    return pl.pallas_call(
        merge_kernel,
        in_specs=[pl.BlockSpec(memory_space=pltpu.VMEM)] * 4,
        out_shape=[
            jax.ShapeDtypeStruct((544, 128), F32),
            jax.ShapeDtypeStruct((544, 128), BF16),
        ],
        cost_estimate=cost(10_000_000, 2_000_000),
        compiler_params=pltpu.CompilerParams(vmem_limit_bytes=6 * 2**20),
        name="merge_stage",
    )(*parts)


def combine_kernel(
    kept_ref, got_ref, norm_ref, gate_ref, proj_ref, out_ref, plane, placed
):
    parts = (kept_ref, got_ref)
    _, scales, denom = merge_stats([r[512:544, :].astype(F32) for r in parts])
    factors = [jnp.broadcast_to(s / denom, (32, 128)) for s in scales]
    plane[...] = norm_ref[...].astype(F32)
    norms = jnp.concatenate(
        [plane[pl.ds(k, 64, stride=2), :] for k in range(2)], axis=1
    ).astype(BF16)
    gate_w = banded(dot(gate_ref[...], by_heads()), 4, 128, 32)
    gate = jax.nn.sigmoid(dot(norms, gate_w))
    proj_w = banded(dot(proj_ref[...], by_heads()), 4, 128, 32)
    total_out = None
    for h in range(8):
        span = slice(h * 64, (h + 1) * 64)
        total = functools.reduce(
            jnp.add,
            [r[span, :].astype(F32) * head_rows(f, h) for r, f in zip(parts, factors)],
        )
        gated = total * gate[:, h * 128 : (h + 1) * 128]
        proj = proj_w[:, h * 128 : (h + 1) * 128]
        high = gated.astype(BF16)
        rest = gated - high.astype(F32)
        middle = rest.astype(BF16)
        low = (rest - middle.astype(F32)).astype(BF16)
        term = dot_nt(low, proj) + dot_nt(middle, proj) + dot_nt(high, proj)
        total_out = term if total_out is None else total_out + term
    for i in range(4):
        for k in range(4):
            placed[pl.ds(k, 16, stride=4), i, :] = total_out[
                i * 16 : (i + 1) * 16, k * 64 : (k + 1) * 64
            ]
    out_ref[...] = placed[...].astype(BF16)


def combine_stage(kept, got, norms, gate, proj):
    return pl.pallas_call(
        combine_kernel,
        in_specs=[pl.BlockSpec(memory_space=pltpu.VMEM)] * 5,
        out_shape=jax.ShapeDtypeStruct((64, 4, 64), BF16),
        scratch_shapes=[pltpu.VMEM((128, 128), F32), pltpu.VMEM((64, 4, 64), F32)],
        cost_estimate=cost(300_000_000, 2_500_000),
        compiler_params=pltpu.CompilerParams(vmem_limit_bytes=10 * 2**20),
        name="combine_stage",
    )(kept, got, norms, gate, proj)


def triangle_kernel(turned_ref, proj_ref, bias_ref, inputs_ref, edge_ref, plane):
    start = pl.program_id(0) * 4
    plane[...] = turned_ref[pl.ds(start, 4)].reshape(512, 128).astype(F32)
    for q in range(4):
        rows = jnp.concatenate(
            [plane[pl.ds(p * 128 + q, 32, stride=4), :] for p in range(4)], axis=0
        ).astype(BF16)
        projected = dot(rows, proj_ref[...])
        inputs_ref[q, :, :384] = projected[:, :384].astype(BF16)
        inputs_ref[q, :, 384:] = jax.nn.sigmoid(projected[:, 384:]).astype(BF16)
        edge_ref[:, q, :] = dot_nt(bias_ref[...], rows).astype(BF16)


def triangle_stage(turned, proj, bias):
    return pl.pallas_call(
        triangle_kernel,
        grid=(8,),
        in_specs=[
            pl.BlockSpec(memory_space=pltpu.VMEM),
            pl.BlockSpec((128, 512), lambda b: (0, 0)),
            pl.BlockSpec((4, 128), lambda b: (0, 0)),
        ],
        out_specs=[
            pl.BlockSpec((4, 128, 512), lambda b: (0, b, 0)),
            pl.BlockSpec((4, 4, 128), lambda b: (0, 0, b)),
        ],
        out_shape=[
            jax.ShapeDtypeStruct((4, 1024, 512), BF16),
            jax.ShapeDtypeStruct((4, 4, 1024), BF16),
        ],
        scratch_shapes=[pltpu.VMEM((512, 128), F32)],
        cost_estimate=cost(1_000_000_000, 6_000_000),
        compiler_params=pltpu.CompilerParams(vmem_limit_bytes=10 * 2**20),
        name="triangle_stage",
    )(turned, proj, bias)


ROUTES = (
    0o71546320, 0o60213574, 0o71453620, 0o46231075, 0o54762013, 0o13207546, 0o64750132, 0o31027654,
    0o02675431, 0o51034276, 0o02647135, 0o70132564, 0o67541302, 0o20316475, 0o57643210, 0o20315467,
    0o12603547, 0o14570236, 0o31607452, 0o46752013, 0o31654720, 0o64302157, 0o20456713, 0o57230146,
    0o32716450, 0o70463125, 0o20135467, 0o57642301, 0o02745631, 0o75210364, 0o13674520, 0o64012357,
)


def left_pairs():
    pairs = []
    for y in range(4):
        for c in range(8):
            route = ROUTES[y * 8 + c]
            for k in range(8):
                target = (route >> (3 * (7 - k))) % 8
                pairs.append(((y * 8 + k) * 8 + c, (c * 4 + y) * 8 + target))
    return pairs


def row_pairs():
    pairs = []
    for r in range(32):
        for c in range(8):
            pairs.append((r * 8 + c, (c * 4 + r // 8) * 8 + r % 8))
    return pairs


def per_device(
    alignment, pair_rep, outer_left, outer_right, outer_proj, outer_bias,
    average_value, average_gate, average_logit, average_out, triangle_proj, triangle_bias,
):
    me = jnp.stack([lax.axis_index(a) for a in ("y", "zl", "x")]).astype(jnp.int32)
    own = prep_stage(alignment, jnp.transpose(outer_left))
    near = lax.all_gather(own, ("zh", "co"), axis=0)
    left_rows = lax.ppermute(near[:, 128:].reshape(512, 128), ALL, left_pairs())
    right, near_norm = right_stage(near, jnp.transpose(outer_right))
    right = lax.all_gather(right, "y", axis=0)
    near_norm, right = lax.optimization_barrier((near_norm, right))
    norm_cols = [near_norm] + [
        lax.ppermute(near_norm, "y", [(c, (c + s) % 4) for c in range(4)])
        for s in range(1, 4)
    ]
    pair_new, turned, logits = pair_stage(
        right, left_rows, pair_rep, outer_proj,
        outer_bias.reshape(1, 128), jnp.transpose(average_logit),
    )
    turned = lax.all_to_all(turned, ROW, 0, 0, tiled=True)
    parts = average_stage(me, logits, average_value, norm_cols)
    moved = {}
    for s in (2, 1, 3):
        moved[s] = lax.ppermute(parts[s], "x", [(c, (c + s) % 4) for c in range(4)])
    norm_own = lax.ppermute(own[:128], ALL, row_pairs())
    kept, sent = merge_stage([parts[0], moved[1], moved[2], moved[3]])
    got = lax.ppermute(sent, "zl", [(0, 1), (1, 0)])
    alignment_update = combine_stage(
        kept, got, norm_own, average_gate, jnp.transpose(average_out)
    )
    turned, alignment_update = lax.optimization_barrier((turned, alignment_update))
    triangle_inputs, edge_bias = triangle_stage(
        turned, triangle_proj, jnp.transpose(triangle_bias)
    )
    return (pair_new, alignment_update, triangle_inputs, edge_bias)


def solution(mesh):
    fine = Mesh(mesh.devices.reshape(4, 4, 2, 2, 4), ALL)
    placed = (P(None, COL + ROW, None), P(ROW, COL, None)) + (P(),) * 10
    return jax.shard_map(
        per_device,
        mesh=fine,
        in_specs=placed,
        out_specs=(
            P(ROW, COL, None),
            P(None, ROW + COL, None),
            P(COL + ROW, None, None),
            P(None, COL + ROW, None),
        ),
        check_vma=False,
    )
```

```python
import functools

import jax
import jax.numpy as jnp
from jax import lax
from jax.experimental import pallas as pl
from jax.experimental.pallas import tpu as pltpu
from jax.sharding import Mesh, PartitionSpec as P


BF16 = jnp.bfloat16
F32 = jnp.float32
ROW = ("y", "zh", "co")
COL = ("zl", "x")
ALL = ROW + COL


def dot(a, b):
    return jnp.dot(a, b, preferred_element_type=F32)


def dot_nt(a, b):
    return lax.dot_general(a, b, (((1,), (1,)), ((), ())), preferred_element_type=F32)


def cost(flops, nbytes, trans=0):
    return pl.CostEstimate(flops=flops, bytes_accessed=nbytes, transcendentals=trans)


def standardize(values):
    widened = values.astype(F32)
    centered = widened - jnp.mean(widened, axis=-1, keepdims=True)
    spread = jnp.mean(centered * centered, axis=-1, keepdims=True)
    return centered * lax.rsqrt(spread + 1e-05)


def iota(shape, dim):
    return lax.broadcasted_iota(jnp.int32, shape, dim)


def picker(rows, cols, rule):
    return jnp.where(rule(iota((rows, cols), 0), iota((rows, cols), 1)), 1.0, 0.0).astype(BF16)


def banded(wide, copies, col_period, col_width):
    tall = jnp.concatenate([wide] * copies, axis=0)
    rows, cols = tall.shape
    here = iota((rows, cols), 0) // wide.shape[0]
    there = (iota((rows, cols), 1) % col_period) // col_width
    return jnp.where(here == there, tall, 0.0).astype(BF16)


def prep_kernel(
    align_ref, left_ref, right_ref, logit_ref, out_ref, right_out, logit_out, wide, plane
):
    right_out[...] = right_ref[...]
    logit_out[...] = logit_ref[...]
    wide[...] = align_ref[...].astype(F32)
    lefts = []
    for t in range(4):
        normed = standardize(wide[:, t, :]).astype(BF16)
        plane[...] = normed.astype(F32)
        out_ref[t * 32 : (t + 1) * 32, :] = jnp.concatenate(
            [plane[pl.ds(0, 32, stride=2), :], plane[pl.ds(1, 32, stride=2), :]], axis=1
        ).astype(BF16)
        lefts.append(dot_nt(normed, left_ref[...]))
    out_ref[128:192, :] = jnp.concatenate(lefts, axis=1).astype(BF16)


def prep_stage(alignment, outer_left, outer_right, average_logit):
    return pl.pallas_call(
        prep_kernel,
        out_shape=[
            jax.ShapeDtypeStruct((192, 128), BF16),
            jax.ShapeDtypeStruct((32, 64), BF16),
            jax.ShapeDtypeStruct((8, 128), BF16),
        ],
        scratch_shapes=[pltpu.VMEM((64, 4, 64), F32), pltpu.VMEM((64, 64), F32)],
        cost_estimate=cost(10_000_000, 100_000),
        compiler_params=pltpu.CompilerParams(vmem_limit_bytes=4 * 2**20),
        name="prep_stage",
    )(alignment, outer_left, outer_right, average_logit)


def right_kernel(near_ref, right_ref, out_ref, norm_ref, wide, tall):
    norms = near_ref[:, :128, :]
    norm_ref[...] = norms
    wide[...] = norms.reshape(1024, 128).astype(F32)
    rows = dot(picker(256, 32, lambda r, c: r // 8 == c), right_ref[...]).astype(BF16)
    rows = dot(rows, picker(64, 512, lambda r, c: c % 64 == r))
    here = iota((256, 512), 0) % 8
    there = iota((256, 512), 1) // 64
    weights = jnp.where(here == there, rows, 0.0).astype(BF16)
    for g in range(8):
        cols = jnp.concatenate(
            [wide[pl.ds(4 * g + k, 32, stride=32), :] for k in range(4)], axis=1
        ).astype(BF16)
        tall[g] = dot_nt(weights, cols)
    for g in range(8):
        group = jnp.concatenate(
            [
                tall[k, (g * 4 + d) * 8 : (g * 4 + d + 1) * 8, :]
                for d in range(4)
                for k in range(8)
            ],
            axis=0,
        )
        out_ref[g] = jnp.transpose(group).astype(BF16)


def right_stage(near, right_w):
    return pl.pallas_call(
        right_kernel,
        in_specs=[pl.BlockSpec(memory_space=pltpu.VMEM)] * 2,
        out_shape=[
            jax.ShapeDtypeStruct((8, 32, 256), BF16),
            jax.ShapeDtypeStruct((8, 128, 128), BF16),
        ],
        scratch_shapes=[pltpu.VMEM((1024, 128), F32), pltpu.VMEM((8, 256, 32), F32)],
        cost_estimate=cost(500_000_000, 500_000),
        compiler_params=pltpu.CompilerParams(vmem_limit_bytes=8 * 2**20),
        name="right_stage",
    )(near, right_w)


def pair_kernel(
    right_ref, left_ref, pair_ref, proj_ref, bias_ref, logit_w_ref,
    new_ref, turned_ref, logit_ref,
    stack, proj, tall, plane, turn,
):
    rows = pair_ref.shape[0]

    @pl.when(pl.program_id(0) == 0)
    def _():
        for g in range(8):
            for y in range(4):
                start = g * 128 + y * 32
                stack[start : start + 32, :] = right_ref[y, g]
        tall[...] = proj_ref[...].astype(F32)
        for d in range(32):
            proj[d * 32 : (d + 1) * 32, :] = tall[pl.ds(d, 32, stride=32), :].astype(BF16)

    for quad in range(rows // 4):
        outer_rows = []
        for p in range(2):
            choose = picker(
                128, 256, lambda r, c: (r // 32 == 2 * p + c // 128) & (r % 32 == c % 32)
            )
            wide = dot(left_ref[quad * 64 : (quad + 1) * 64, :], choose)
            outer = dot(stack[...], banded(wide, 4, 128, 32)).astype(BF16)
            for k in range(2):
                outer_rows.append(
                    jnp.concatenate(
                        [
                            outer[g * 128 : (g + 1) * 128, k * 128 : (k + 1) * 128]
                            for g in range(8)
                        ],
                        axis=1,
                    )
                )
        update = jnp.concatenate([dot(rows_i, proj[...]) for rows_i in outer_rows], axis=0)
        four = slice(quad * 4, (quad + 1) * 4)
        pair = pair_ref[four].reshape(512, 128).astype(F32)
        fresh = (pair + update * (1.0 / 64.0) + bias_ref[...]).astype(BF16)
        new_ref[four] = fresh.reshape(4, 128, 128)
        normed = standardize(fresh)
        normed_low = normed.astype(BF16)
        for i in range(4):
            logit_ref[quad * 4 + i] = dot_nt(
                logit_w_ref[...], normed_low[i * 128 : (i + 1) * 128]
            )
        plane[quad] = normed
        for i in range(4):
            for q in range(4):
                turn[pl.ds((quad * 4 + i) * 4 + q, 32, stride=4 * rows), :] = plane[
                    quad, pl.ds(i * 128 + q, 32, stride=4), :
                ]
    turned_ref[...] = turn[...].reshape(32, 4 * rows, 128).astype(BF16)


def pair_stage(right, left, pair_rep, proj, bias, logit_w):
    block = 8
    steps = 32 // block
    return pl.pallas_call(
        pair_kernel,
        grid=(steps,),
        in_specs=[
            pl.BlockSpec((4, 8, 32, 256), lambda b: (0, 0, 0, 0)),
            pl.BlockSpec((16 * block, 128), lambda b: (b, 0)),
            pl.BlockSpec((block, 128, 128), lambda b: (b, 0, 0)),
            pl.BlockSpec((1024, 128), lambda b: (0, 0)),
            pl.BlockSpec((1, 128), lambda b: (0, 0)),
            pl.BlockSpec((8, 128), lambda b: (0, 0)),
        ],
        out_specs=[
            pl.BlockSpec((block, 128, 128), lambda b: (b, 0, 0)),
            pl.BlockSpec((32, 4 * block, 128), lambda b: (0, b, 0)),
            pl.BlockSpec((block, 8, 128), lambda b: (b, 0, 0)),
        ],
        out_shape=[
            jax.ShapeDtypeStruct((32, 128, 128), BF16),
            jax.ShapeDtypeStruct((32, 128, 128), BF16),
            jax.ShapeDtypeStruct((32, 8, 128), F32),
        ],
        scratch_shapes=[
            pltpu.VMEM((1024, 256), BF16),
            pltpu.VMEM((1024, 128), BF16),
            pltpu.VMEM((1024, 128), F32),
            pltpu.VMEM((block // 4, 512, 128), F32),
            pltpu.VMEM((block * 128, 128), F32),
        ],
        cost_estimate=cost(8_000_000_000, 6_000_000),
        compiler_params=pltpu.CompilerParams(vmem_limit_bytes=26 * 2**20),
        name="pair_stage",
    )(right, left, pair_rep, proj, bias, logit_w)


def by_heads():
    return picker(256, 1024, lambda r, c: (r // 32 == c // 128) & (r % 32 == c % 32))


def pack_stats(denom, peak):
    high = denom.astype(BF16).astype(F32)
    lane = iota((denom.shape[0], 128), 1)
    return jnp.where(
        lane == 0,
        high,
        jnp.where(lane == 1, denom - high, jnp.where(lane == 2, peak, 0.0)),
    )


def average_kernel(me_ref, logit_ref, value_ref, *refs):
    norms, outs, (wide, spare, summed, parts) = refs[:4], refs[4:8], refs[8:]
    me_y, me_z, me_x = me_ref[0], me_ref[1], me_ref[2]
    logits = logit_ref[...].reshape(256, 128)
    peak = jnp.max(logits, axis=1, keepdims=True).astype(BF16).astype(F32)
    weights = jnp.exp(logits - peak).astype(BF16).astype(F32)
    stats = pack_stats(jnp.sum(weights, axis=1, keepdims=True), peak)
    spare[...] = weights
    by_head = jnp.concatenate(
        [spare[pl.ds(h, 32, stride=8), :] for h in range(8)], axis=0
    ).astype(BF16)
    for s in range(4):
        start = pl.multiple_of(lax.rem(me_y + 4 - s, 4) * 1024, 1024)
        wide[pl.ds(start, 1024), :] = norms[s][...].reshape(1024, 128).astype(F32)
    for g in range(16):
        cols = jnp.concatenate(
            [wide[pl.ds(2 * g + k, 128, stride=32), :] for k in range(2)], axis=1
        ).astype(BF16)
        summed[g] = dot(by_head, cols).astype(BF16)
    spare[...] = stats
    targets = [
        [lax.rem(me_z + k, 2) * 4 + lax.rem(me_x + s, 4) for k in range(2)] for s in range(4)
    ]
    for s in range(4):
        for k in range(2):
            start = pl.multiple_of(targets[s][k] * 32, 32)
            outs[s][k, 512:544, :] = spare[pl.ds(start, 32), :].astype(BF16)
    value_w = banded(dot(value_ref[...], by_heads()), 4, 128, 32)
    for h in range(8):
        rows = summed[:, h * 32 : (h + 1) * 32, :].reshape(512, 256)
        parts[...] = dot(rows, value_w[:, h * 128 : (h + 1) * 128])
        for s in range(4):
            for k in range(2):
                for i in range(4):
                    start = h * 64 + i * 16
                    outs[s][k, start : start + 16, :] = parts[
                        pl.ds(targets[s][k] * 4 + i, 16, stride=32), :
                    ].astype(BF16)


def average_stage(me, logits, value, norms):
    return pl.pallas_call(
        average_kernel,
        in_specs=[
            pl.BlockSpec(memory_space=pltpu.SMEM),
        ]
        + [pl.BlockSpec(memory_space=pltpu.VMEM)] * 6,
        out_shape=[jax.ShapeDtypeStruct((2, 544, 128), BF16)] * 4,
        scratch_shapes=[
            pltpu.VMEM((4096, 128), F32),
            pltpu.VMEM((256, 128), F32),
            pltpu.VMEM((16, 256, 256), BF16),
            pltpu.VMEM((512, 128), F32),
        ],
        cost_estimate=cost(2_000_000_000, 3_000_000),
        compiler_params=pltpu.CompilerParams(vmem_limit_bytes=16 * 2**20),
        name="average_stage",
    )(me, logits, value, *norms)


def merge_stats(stats):
    denoms = [st[:, 0:1] + st[:, 1:2] for st in stats]
    peaks = [st[:, 2:3] for st in stats]
    top = functools.reduce(jnp.maximum, peaks)
    scales = [jnp.exp(peak - top) for peak in peaks]
    denom = functools.reduce(jnp.add, [s * d for s, d in zip(scales, denoms)])
    return top, scales, denom


def head_rows(factor, h):
    return jnp.concatenate(
        [jnp.broadcast_to(factor[i * 8 + h : i * 8 + h + 1], (16, 128)) for i in range(4)],
        axis=0,
    )


def merge_kernel(a_ref, b_ref, c_ref, d_ref, keep_ref, send_ref):
    sources = (a_ref, b_ref, c_ref, d_ref)
    for k, out in ((1, send_ref), (0, keep_ref)):
        top, scales, denom = merge_stats([r[k, 512:544, :].astype(F32) for r in sources])
        out[512:544, :] = pack_stats(denom, top).astype(out.dtype)
        factors = [jnp.broadcast_to(s, (32, 128)) for s in scales]
        for h in range(8):
            span = slice(h * 64, (h + 1) * 64)
            terms = [
                r[k, span, :].astype(F32) * head_rows(f, h) for r, f in zip(sources, factors)
            ]
            out[span, :] = ((terms[0] + terms[1]) + (terms[2] + terms[3])).astype(out.dtype)


def merge_stage(parts):
    return pl.pallas_call(
        merge_kernel,
        in_specs=[pl.BlockSpec(memory_space=pltpu.VMEM)] * 4,
        out_shape=[
            jax.ShapeDtypeStruct((544, 128), F32),
            jax.ShapeDtypeStruct((544, 128), BF16),
        ],
        cost_estimate=cost(10_000_000, 2_000_000),
        compiler_params=pltpu.CompilerParams(vmem_limit_bytes=6 * 2**20),
        name="merge_stage",
    )(*parts)


def combine_kernel(
    kept_ref, got_ref, norm_ref, gate_ref, proj_ref, out_ref, plane, placed
):
    parts = (kept_ref, got_ref)
    _, scales, denom = merge_stats([r[512:544, :].astype(F32) for r in parts])
    factors = [jnp.broadcast_to(s / denom, (32, 128)) for s in scales]
    plane[...] = norm_ref[...].astype(F32)
    norms = jnp.concatenate(
        [plane[pl.ds(k, 64, stride=2), :] for k in range(2)], axis=1
    ).astype(BF16)
    gate_w = banded(dot(gate_ref[...], by_heads()), 4, 128, 32)
    gate = jax.nn.sigmoid(dot(norms, gate_w))
    proj_w = banded(dot(proj_ref[...], by_heads()), 4, 128, 32)
    total_out = None
    for h in range(8):
        span = slice(h * 64, (h + 1) * 64)
        total = functools.reduce(
            jnp.add,
            [r[span, :].astype(F32) * head_rows(f, h) for r, f in zip(parts, factors)],
        )
        gated = total * gate[:, h * 128 : (h + 1) * 128]
        proj = proj_w[:, h * 128 : (h + 1) * 128]
        high = gated.astype(BF16)
        rest = gated - high.astype(F32)
        middle = rest.astype(BF16)
        low = (rest - middle.astype(F32)).astype(BF16)
        term = dot_nt(low, proj) + dot_nt(middle, proj) + dot_nt(high, proj)
        total_out = term if total_out is None else total_out + term
    for i in range(4):
        for k in range(4):
            placed[pl.ds(k, 16, stride=4), i, :] = total_out[
                i * 16 : (i + 1) * 16, k * 64 : (k + 1) * 64
            ]
    out_ref[...] = placed[...].astype(BF16)


def combine_stage(kept, got, norms, gate, proj):
    return pl.pallas_call(
        combine_kernel,
        in_specs=[pl.BlockSpec(memory_space=pltpu.VMEM)] * 5,
        out_shape=jax.ShapeDtypeStruct((64, 4, 64), BF16),
        scratch_shapes=[pltpu.VMEM((128, 128), F32), pltpu.VMEM((64, 4, 64), F32)],
        cost_estimate=cost(300_000_000, 2_500_000),
        compiler_params=pltpu.CompilerParams(vmem_limit_bytes=10 * 2**20),
        name="combine_stage",
    )(kept, got, norms, gate, proj)


def triangle_kernel(turned_ref, proj_ref, bias_ref, inputs_ref, edge_ref, plane):
    start = pl.program_id(0) * 8
    plane[...] = turned_ref[pl.ds(start, 8)].reshape(1024, 128).astype(F32)
    for q in range(4):
        rows = jnp.concatenate(
            [plane[pl.ds(p * 128 + q, 32, stride=4), :] for p in range(8)], axis=0
        ).astype(BF16)
        projected = dot(rows, proj_ref[...])
        inputs_ref[q, :, :384] = projected[:, :384].astype(BF16)
        inputs_ref[q, :, 384:] = jax.nn.sigmoid(projected[:, 384:]).astype(BF16)
        edge_ref[:, q, :] = dot_nt(bias_ref[...], rows).astype(BF16)


def triangle_stage(turned, proj, bias):
    return pl.pallas_call(
        triangle_kernel,
        grid=(4,),
        in_specs=[
            pl.BlockSpec(memory_space=pltpu.VMEM),
            pl.BlockSpec((128, 512), lambda b: (0, 0)),
            pl.BlockSpec((4, 128), lambda b: (0, 0)),
        ],
        out_specs=[
            pl.BlockSpec((4, 256, 512), lambda b: (0, b, 0)),
            pl.BlockSpec((4, 4, 256), lambda b: (0, 0, b)),
        ],
        out_shape=[
            jax.ShapeDtypeStruct((4, 1024, 512), BF16),
            jax.ShapeDtypeStruct((4, 4, 1024), BF16),
        ],
        scratch_shapes=[pltpu.VMEM((1024, 128), F32)],
        cost_estimate=cost(1_000_000_000, 6_000_000),
        compiler_params=pltpu.CompilerParams(vmem_limit_bytes=14 * 2**20),
        name="triangle_stage",
    )(turned, proj, bias)


ROUTES = (
    0o71546320, 0o60213574, 0o71453620, 0o46231075, 0o54762013, 0o13207546, 0o64750132, 0o31027654,
    0o02675431, 0o51034276, 0o02647135, 0o70132564, 0o67541302, 0o20316475, 0o57643210, 0o20315467,
    0o12603547, 0o14570236, 0o31607452, 0o46752013, 0o31654720, 0o64302157, 0o20456713, 0o57230146,
    0o32716450, 0o70463125, 0o20135467, 0o57642301, 0o02745631, 0o75210364, 0o13674520, 0o64012357,
)


def left_pairs():
    pairs = []
    for y in range(4):
        for c in range(8):
            route = ROUTES[y * 8 + c]
            for k in range(8):
                target = (route >> (3 * (7 - k))) % 8
                pairs.append(((y * 8 + k) * 8 + c, (c * 4 + y) * 8 + target))
    return pairs


def row_pairs():
    pairs = []
    for r in range(32):
        for c in range(8):
            pairs.append((r * 8 + c, (c * 4 + r // 8) * 8 + r % 8))
    return pairs


def per_device(
    alignment, pair_rep, outer_left, outer_right, outer_proj, outer_bias,
    average_value, average_gate, average_logit, average_out, triangle_proj, triangle_bias,
):
    me = jnp.stack([lax.axis_index(a) for a in ("y", "zl", "x")]).astype(jnp.int32)
    own, right_w, logit_w = prep_stage(
        alignment, jnp.transpose(outer_left), jnp.transpose(outer_right),
        jnp.transpose(average_logit),
    )
    near = lax.all_gather(own, ("zh", "co"), axis=0)
    left_rows = lax.ppermute(near[:, 128:].reshape(512, 128), ALL, left_pairs())
    right, near_norm = right_stage(near, right_w)
    right = lax.all_to_all(jnp.broadcast_to(right[None], (4, 8, 32, 256)), "y", 0, 0, tiled=True)
    near_norm, right = lax.optimization_barrier((near_norm, right))
    norm_cols = [near_norm] + [
        lax.ppermute(near_norm, "y", [(c, (c + s) % 4) for c in range(4)])
        for s in range(1, 4)
    ]
    pair_new, turned, logits = pair_stage(
        right, left_rows, pair_rep, outer_proj,
        outer_bias.reshape(1, 128), logit_w,
    )
    turned = lax.all_to_all(turned, ROW, 0, 0, tiled=True)
    parts = average_stage(me, logits, average_value, norm_cols)
    moved = {}
    for s in (2, 1, 3):
        moved[s] = lax.ppermute(parts[s], "x", [(c, (c + s) % 4) for c in range(4)])
    norm_own = lax.ppermute(own[:128], ALL, row_pairs())
    kept, sent = merge_stage([parts[0], moved[1], moved[2], moved[3]])
    got = lax.ppermute(sent, "zl", [(0, 1), (1, 0)])
    turned, kept = lax.optimization_barrier((turned, kept))
    triangle_inputs, edge_bias = triangle_stage(
        turned, triangle_proj, jnp.transpose(triangle_bias)
    )
    norm_own, edge_bias = lax.optimization_barrier((norm_own, edge_bias))
    alignment_update = combine_stage(
        kept, got, norm_own, average_gate, jnp.transpose(average_out)
    )
    return (pair_new, alignment_update, triangle_inputs, edge_bias)


def solution(mesh):
    fine = Mesh(mesh.devices.reshape(4, 4, 2, 2, 4), ALL)
    placed = (P(None, COL + ROW, None), P(ROW, COL, None)) + (P(),) * 10
    return jax.shard_map(
        per_device,
        mesh=fine,
        in_specs=placed,
        out_specs=(
            P(ROW, COL, None),
            P(None, ROW + COL, None),
            P(COL + ROW, None, None),
            P(None, COL + ROW, None),
        ),
        check_vma=False,
    )
```

```python
import functools

import jax
import jax.numpy as jnp
from jax import lax
from jax.experimental import pallas as pl
from jax.experimental.pallas import tpu as pltpu
from jax.sharding import Mesh, PartitionSpec as P


BF16 = jnp.bfloat16
F32 = jnp.float32
ROW = ("y", "zh", "co")
COL = ("zl", "x")
ALL = ROW + COL


def dot(a, b):
    return jnp.dot(a, b, preferred_element_type=F32)


def dot_nt(a, b):
    return lax.dot_general(a, b, (((1,), (1,)), ((), ())), preferred_element_type=F32)


def cost(flops, nbytes, trans=0):
    return pl.CostEstimate(flops=flops, bytes_accessed=nbytes, transcendentals=trans)


def standardize(values):
    widened = values.astype(F32)
    centered = widened - jnp.mean(widened, axis=-1, keepdims=True)
    spread = jnp.mean(centered * centered, axis=-1, keepdims=True)
    return centered * lax.rsqrt(spread + 1e-05)


def iota(shape, dim):
    return lax.broadcasted_iota(jnp.int32, shape, dim)


def picker(rows, cols, rule):
    return jnp.where(rule(iota((rows, cols), 0), iota((rows, cols), 1)), 1.0, 0.0).astype(BF16)


def banded(wide, copies, col_period, col_width):
    tall = jnp.concatenate([wide] * copies, axis=0)
    rows, cols = tall.shape
    here = iota((rows, cols), 0) // wide.shape[0]
    there = (iota((rows, cols), 1) % col_period) // col_width
    return jnp.where(here == there, tall, 0.0).astype(BF16)


def prep_kernel(align_ref, left_ref, out_ref, wide, plane):
    wide[...] = align_ref[...].astype(F32)
    lefts = []
    for t in range(4):
        normed = standardize(wide[:, t, :]).astype(BF16)
        plane[...] = normed.astype(F32)
        out_ref[t * 32 : (t + 1) * 32, :] = jnp.concatenate(
            [plane[pl.ds(0, 32, stride=2), :], plane[pl.ds(1, 32, stride=2), :]], axis=1
        ).astype(BF16)
        lefts.append(dot_nt(normed, left_ref[...]))
    out_ref[128:192, :] = jnp.concatenate(lefts, axis=1).astype(BF16)


def prep_stage(alignment, outer_left):
    return pl.pallas_call(
        prep_kernel,
        out_shape=jax.ShapeDtypeStruct((192, 128), BF16),
        scratch_shapes=[pltpu.VMEM((64, 4, 64), F32), pltpu.VMEM((64, 64), F32)],
        cost_estimate=cost(10_000_000, 100_000),
        compiler_params=pltpu.CompilerParams(vmem_limit_bytes=4 * 2**20),
        name="prep_stage",
    )(alignment, outer_left)


def right_kernel(near_ref, right_ref, out_ref, norm_ref, wide, tall):
    norms = near_ref[:, :128, :]
    norm_ref[...] = norms
    wide[...] = norms.reshape(1024, 128).astype(F32)
    rows = dot(picker(256, 32, lambda r, c: r // 8 == c), right_ref[...]).astype(BF16)
    rows = dot(rows, picker(64, 512, lambda r, c: c % 64 == r))
    here = iota((256, 512), 0) % 8
    there = iota((256, 512), 1) // 64
    weights = jnp.where(here == there, rows, 0.0).astype(BF16)
    for g in range(8):
        cols = jnp.concatenate(
            [wide[pl.ds(4 * g + k, 32, stride=32), :] for k in range(4)], axis=1
        ).astype(BF16)
        tall[g] = dot_nt(weights, cols)
    for g in range(8):
        group = jnp.concatenate(
            [
                tall[k, (g * 4 + d) * 8 : (g * 4 + d + 1) * 8, :]
                for d in range(4)
                for k in range(8)
            ],
            axis=0,
        )
        out_ref[g] = jnp.transpose(group).astype(BF16)


def right_stage(near, right_w):
    return pl.pallas_call(
        right_kernel,
        in_specs=[pl.BlockSpec(memory_space=pltpu.VMEM)] * 2,
        out_shape=[
            jax.ShapeDtypeStruct((8, 32, 256), BF16),
            jax.ShapeDtypeStruct((8, 128, 128), BF16),
        ],
        scratch_shapes=[pltpu.VMEM((1024, 128), F32), pltpu.VMEM((8, 256, 32), F32)],
        cost_estimate=cost(8_000_000_000, 12_000_000),
        compiler_params=pltpu.CompilerParams(vmem_limit_bytes=8 * 2**20),
        name="right_stage",
    )(near, right_w)


def pair_kernel(
    me_ref, right_0, right_1, right_2, right_3, left_ref, pair_ref, proj_ref, bias_ref, logit_w_ref,
    new_ref, turned_ref, logit_ref,
    stack, proj, tall, plane, turn,
):
    rows = pair_ref.shape[0]

    @pl.when(pl.program_id(0) == 0)
    def _():
        for s, right_ref in enumerate((right_0, right_1, right_2, right_3)):
            near = lax.rem(me_ref[0] + 4 - s, 4) * 32
            for g in range(8):
                start = pl.multiple_of(g * 128 + near, 32)
                stack[pl.ds(start, 32), :] = right_ref[g]
        tall[...] = proj_ref[...].astype(F32)
        for d in range(32):
            proj[d * 32 : (d + 1) * 32, :] = tall[pl.ds(d, 32, stride=32), :].astype(BF16)

    for quad in range(rows // 4):
        outer_rows = []
        for p in range(2):
            choose = picker(
                128, 256, lambda r, c: (r // 32 == 2 * p + c // 128) & (r % 32 == c % 32)
            )
            wide = dot(left_ref[quad * 64 : (quad + 1) * 64, :], choose)
            outer = dot(stack[...], banded(wide, 4, 128, 32)).astype(BF16)
            for k in range(2):
                outer_rows.append(
                    jnp.concatenate(
                        [
                            outer[g * 128 : (g + 1) * 128, k * 128 : (k + 1) * 128]
                            for g in range(8)
                        ],
                        axis=1,
                    )
                )
        update = jnp.concatenate([dot(rows_i, proj[...]) for rows_i in outer_rows], axis=0)
        four = slice(quad * 4, (quad + 1) * 4)
        pair = pair_ref[four].reshape(512, 128).astype(F32)
        fresh = (pair + update * (1.0 / 64.0) + bias_ref[...]).astype(BF16)
        new_ref[four] = fresh.reshape(4, 128, 128)
        normed = standardize(fresh)
        normed_low = normed.astype(BF16)
        for i in range(4):
            logit_ref[quad * 4 + i] = dot_nt(
                logit_w_ref[...], normed_low[i * 128 : (i + 1) * 128]
            )
        plane[quad] = normed
        for i in range(4):
            for q in range(4):
                turn[pl.ds((quad * 4 + i) * 4 + q, 32, stride=4 * rows), :] = plane[
                    quad, pl.ds(i * 128 + q, 32, stride=4), :
                ]
    turned_ref[...] = turn[...].reshape(32, 4 * rows, 128).astype(BF16)


def pair_stage(me, right, left, pair_rep, proj, bias, logit_w):
    block = 8
    steps = 32 // block
    return pl.pallas_call(
        pair_kernel,
        grid=(steps,),
        in_specs=[
            pl.BlockSpec(memory_space=pltpu.SMEM),
        ]
        + [pl.BlockSpec((8, 32, 256), lambda b: (0, 0, 0))] * 4
        + [
            pl.BlockSpec((16 * block, 128), lambda b: (b, 0)),
            pl.BlockSpec((block, 128, 128), lambda b: (b, 0, 0)),
            pl.BlockSpec((1024, 128), lambda b: (0, 0)),
            pl.BlockSpec((1, 128), lambda b: (0, 0)),
            pl.BlockSpec((8, 128), lambda b: (0, 0)),
        ],
        out_specs=[
            pl.BlockSpec((block, 128, 128), lambda b: (b, 0, 0)),
            pl.BlockSpec((32, 4 * block, 128), lambda b: (0, b, 0)),
            pl.BlockSpec((block, 8, 128), lambda b: (b, 0, 0)),
        ],
        out_shape=[
            jax.ShapeDtypeStruct((32, 128, 128), BF16),
            jax.ShapeDtypeStruct((32, 128, 128), BF16),
            jax.ShapeDtypeStruct((32, 8, 128), F32),
        ],
        scratch_shapes=[
            pltpu.VMEM((1024, 256), BF16),
            pltpu.VMEM((1024, 128), BF16),
            pltpu.VMEM((1024, 128), F32),
            pltpu.VMEM((block // 4, 512, 128), F32),
            pltpu.VMEM((block * 128, 128), F32),
        ],
        cost_estimate=cost(8_000_000_000, 6_000_000),
        compiler_params=pltpu.CompilerParams(vmem_limit_bytes=26 * 2**20),
        name="pair_stage",
    )(me, *right, left, pair_rep, proj, bias, logit_w)


def by_heads():
    return picker(256, 1024, lambda r, c: (r // 32 == c // 128) & (r % 32 == c % 32))


def pack_stats(denom, peak):
    high = denom.astype(BF16).astype(F32)
    lane = iota((denom.shape[0], 128), 1)
    return jnp.where(
        lane == 0,
        high,
        jnp.where(lane == 1, denom - high, jnp.where(lane == 2, peak, 0.0)),
    )


def average_kernel(me_ref, logit_ref, value_ref, *refs):
    norms, outs, (wide, spare, summed, parts) = refs[:4], refs[4:8], refs[8:]
    me_y, me_z, me_x = me_ref[0], me_ref[1], me_ref[2]
    logits = logit_ref[...].reshape(256, 128)
    peak = jnp.max(logits, axis=1, keepdims=True).astype(BF16).astype(F32)
    weights = jnp.exp(logits - peak).astype(BF16).astype(F32)
    stats = pack_stats(jnp.sum(weights, axis=1, keepdims=True), peak)
    spare[...] = weights
    by_head = jnp.concatenate(
        [spare[pl.ds(h, 32, stride=8), :] for h in range(8)], axis=0
    ).astype(BF16)
    for s in range(4):
        start = pl.multiple_of(lax.rem(me_y + 4 - s, 4) * 1024, 1024)
        wide[pl.ds(start, 1024), :] = norms[s][...].reshape(1024, 128).astype(F32)
    for g in range(16):
        cols = jnp.concatenate(
            [wide[pl.ds(2 * g + k, 128, stride=32), :] for k in range(2)], axis=1
        ).astype(BF16)
        summed[g] = dot(by_head, cols).astype(BF16)
    spare[...] = stats
    targets = [
        [lax.rem(me_z + k, 2) * 4 + lax.rem(me_x + s, 4) for k in range(2)] for s in range(4)
    ]
    for s in range(4):
        for k in range(2):
            start = pl.multiple_of(targets[s][k] * 32, 32)
            outs[s][k, 512:544, :] = spare[pl.ds(start, 32), :].astype(BF16)
    value_w = banded(dot(value_ref[...], by_heads()), 4, 128, 32)
    for h in range(8):
        rows = summed[:, h * 32 : (h + 1) * 32, :].reshape(512, 256)
        parts[...] = dot(rows, value_w[:, h * 128 : (h + 1) * 128])
        for s in range(4):
            for k in range(2):
                for i in range(4):
                    start = h * 64 + i * 16
                    outs[s][k, start : start + 16, :] = parts[
                        pl.ds(targets[s][k] * 4 + i, 16, stride=32), :
                    ].astype(BF16)


def average_stage(me, logits, value, norms):
    return pl.pallas_call(
        average_kernel,
        in_specs=[
            pl.BlockSpec(memory_space=pltpu.SMEM),
        ]
        + [pl.BlockSpec(memory_space=pltpu.VMEM)] * 6,
        out_shape=[jax.ShapeDtypeStruct((2, 544, 128), BF16)] * 4,
        scratch_shapes=[
            pltpu.VMEM((4096, 128), F32),
            pltpu.VMEM((256, 128), F32),
            pltpu.VMEM((16, 256, 256), BF16),
            pltpu.VMEM((512, 128), F32),
        ],
        cost_estimate=cost(2_000_000_000, 3_000_000),
        compiler_params=pltpu.CompilerParams(vmem_limit_bytes=16 * 2**20),
        name="average_stage",
    )(me, logits, value, *norms)


def merge_stats(stats):
    denoms = [st[:, 0:1] + st[:, 1:2] for st in stats]
    peaks = [st[:, 2:3] for st in stats]
    top = functools.reduce(jnp.maximum, peaks)
    scales = [jnp.exp(peak - top) for peak in peaks]
    denom = functools.reduce(jnp.add, [s * d for s, d in zip(scales, denoms)])
    return top, scales, denom


def head_rows(factor, h):
    return jnp.concatenate(
        [jnp.broadcast_to(factor[i * 8 + h : i * 8 + h + 1], (16, 128)) for i in range(4)],
        axis=0,
    )


def merge_kernel(a_ref, b_ref, c_ref, d_ref, keep_ref, send_ref):
    sources = (a_ref, b_ref, c_ref, d_ref)
    for k, out in ((1, send_ref), (0, keep_ref)):
        top, scales, denom = merge_stats([r[k, 512:544, :].astype(F32) for r in sources])
        out[512:544, :] = pack_stats(denom, top).astype(out.dtype)
        factors = [jnp.broadcast_to(s, (32, 128)) for s in scales]
        for h in range(8):
            span = slice(h * 64, (h + 1) * 64)
            terms = [
                r[k, span, :].astype(F32) * head_rows(f, h) for r, f in zip(sources, factors)
            ]
            out[span, :] = ((terms[0] + terms[1]) + (terms[2] + terms[3])).astype(out.dtype)


def merge_stage(parts):
    return pl.pallas_call(
        merge_kernel,
        in_specs=[pl.BlockSpec(memory_space=pltpu.VMEM)] * 4,
        out_shape=[
            jax.ShapeDtypeStruct((544, 128), F32),
            jax.ShapeDtypeStruct((544, 128), BF16),
        ],
        cost_estimate=cost(10_000_000, 2_000_000),
        compiler_params=pltpu.CompilerParams(vmem_limit_bytes=6 * 2**20),
        name="merge_stage",
    )(*parts)


def combine_kernel(
    kept_ref, got_ref, norm_ref, gate_ref, proj_ref, out_ref, plane, placed
):
    parts = (kept_ref, got_ref)
    _, scales, denom = merge_stats([r[512:544, :].astype(F32) for r in parts])
    factors = [jnp.broadcast_to(s / denom, (32, 128)) for s in scales]
    plane[...] = norm_ref[...].astype(F32)
    norms = jnp.concatenate(
        [plane[pl.ds(k, 64, stride=2), :] for k in range(2)], axis=1
    ).astype(BF16)
    gate_w = banded(dot(gate_ref[...], by_heads()), 4, 128, 32)
    gate = jax.nn.sigmoid(dot(norms, gate_w))
    proj_w = banded(dot(proj_ref[...], by_heads()), 4, 128, 32)
    total_out = None
    for h in range(8):
        span = slice(h * 64, (h + 1) * 64)
        total = functools.reduce(
            jnp.add,
            [r[span, :].astype(F32) * head_rows(f, h) for r, f in zip(parts, factors)],
        )
        gated = total * gate[:, h * 128 : (h + 1) * 128]
        proj = proj_w[:, h * 128 : (h + 1) * 128]
        high = gated.astype(BF16)
        rest = gated - high.astype(F32)
        middle = rest.astype(BF16)
        low = (rest - middle.astype(F32)).astype(BF16)
        term = dot_nt(low, proj) + dot_nt(middle, proj) + dot_nt(high, proj)
        total_out = term if total_out is None else total_out + term
    for i in range(4):
        for k in range(4):
            placed[pl.ds(k, 16, stride=4), i, :] = total_out[
                i * 16 : (i + 1) * 16, k * 64 : (k + 1) * 64
            ]
    out_ref[...] = placed[...].astype(BF16)


def combine_stage(kept, got, norms, gate, proj):
    return pl.pallas_call(
        combine_kernel,
        in_specs=[pl.BlockSpec(memory_space=pltpu.VMEM)] * 5,
        out_shape=jax.ShapeDtypeStruct((64, 4, 64), BF16),
        scratch_shapes=[pltpu.VMEM((128, 128), F32), pltpu.VMEM((64, 4, 64), F32)],
        cost_estimate=cost(300_000_000, 2_500_000),
        compiler_params=pltpu.CompilerParams(vmem_limit_bytes=10 * 2**20),
        name="combine_stage",
    )(kept, got, norms, gate, proj)


def triangle_kernel(turned_ref, proj_ref, bias_ref, inputs_ref, edge_ref, plane):
    start = pl.program_id(0) * 8
    plane[...] = turned_ref[pl.ds(start, 8)].reshape(1024, 128).astype(F32)
    for q in range(4):
        rows = jnp.concatenate(
            [plane[pl.ds(p * 128 + q, 32, stride=4), :] for p in range(8)], axis=0
        ).astype(BF16)
        projected = dot(rows, proj_ref[...])
        inputs_ref[q, :, :384] = projected[:, :384].astype(BF16)
        inputs_ref[q, :, 384:] = jax.nn.sigmoid(projected[:, 384:]).astype(BF16)
        edge_ref[:, q, :] = dot_nt(bias_ref[...], rows).astype(BF16)


def triangle_stage(turned, proj, bias):
    return pl.pallas_call(
        triangle_kernel,
        grid=(4,),
        in_specs=[
            pl.BlockSpec(memory_space=pltpu.VMEM),
            pl.BlockSpec((128, 512), lambda b: (0, 0)),
            pl.BlockSpec((4, 128), lambda b: (0, 0)),
        ],
        out_specs=[
            pl.BlockSpec((4, 256, 512), lambda b: (0, b, 0)),
            pl.BlockSpec((4, 4, 256), lambda b: (0, 0, b)),
        ],
        out_shape=[
            jax.ShapeDtypeStruct((4, 1024, 512), BF16),
            jax.ShapeDtypeStruct((4, 4, 1024), BF16),
        ],
        scratch_shapes=[pltpu.VMEM((1024, 128), F32)],
        cost_estimate=cost(1_000_000_000, 6_000_000),
        compiler_params=pltpu.CompilerParams(vmem_limit_bytes=14 * 2**20),
        name="triangle_stage",
    )(turned, proj, bias)


ROUTES = (
    0o71546320, 0o60213574, 0o71453620, 0o46231075, 0o54762013, 0o13207546, 0o64750132, 0o31027654,
    0o02675431, 0o51034276, 0o02647135, 0o70132564, 0o67541302, 0o20316475, 0o57643210, 0o20315467,
    0o12603547, 0o14570236, 0o31607452, 0o46752013, 0o31654720, 0o64302157, 0o20456713, 0o57230146,
    0o32716450, 0o70463125, 0o20135467, 0o57642301, 0o02745631, 0o75210364, 0o13674520, 0o64012357,
)


def left_pairs():
    pairs = []
    for y in range(4):
        for c in range(8):
            route = ROUTES[y * 8 + c]
            for k in range(8):
                target = (route >> (3 * (7 - k))) % 8
                pairs.append(((y * 8 + k) * 8 + c, (c * 4 + y) * 8 + target))
    return pairs


def row_pairs():
    pairs = []
    for r in range(32):
        for c in range(8):
            pairs.append((r * 8 + c, (c * 4 + r // 8) * 8 + r % 8))
    return pairs


def per_device(
    alignment, pair_rep, outer_left, outer_right, outer_proj, outer_bias,
    average_value, average_gate, average_logit, average_out, triangle_proj, triangle_bias,
):
    me = jnp.stack([lax.axis_index(a) for a in ("y", "zl", "x")]).astype(jnp.int32)
    own = prep_stage(alignment, jnp.transpose(outer_left))
    near = lax.all_gather(own, ("zh", "co"), axis=0)
    left_rows = lax.ppermute(near[:, 128:].reshape(512, 128), ALL, left_pairs())
    right, near_norm = right_stage(near, jnp.transpose(outer_right))
    right_got, norm_got = {}, {}
    for s in (2, 1, 3):
        right_got[s] = lax.ppermute(right, "y", [(c, (c + s) % 4) for c in range(4)])
    near_norm, right_got = lax.optimization_barrier((near_norm, right_got))
    for s in (2, 1, 3):
        norm_got[s] = lax.ppermute(near_norm, "y", [(c, (c + s) % 4) for c in range(4)])
    right_cols = [right] + [right_got[s] for s in (1, 2, 3)]
    norm_cols = [near_norm] + [norm_got[s] for s in (1, 2, 3)]
    pair_new, turned, logits = pair_stage(
        me, right_cols, left_rows, pair_rep, outer_proj,
        outer_bias.reshape(1, 128), jnp.transpose(average_logit),
    )
    turned = lax.all_to_all(turned, ROW, 0, 0, tiled=True)
    parts = average_stage(me, logits, average_value, norm_cols)
    moved = {}
    for s in (2, 1, 3):
        moved[s] = lax.ppermute(parts[s], "x", [(c, (c + s) % 4) for c in range(4)])
    norm_own = lax.ppermute(own[:128], ALL, row_pairs())
    kept, sent = merge_stage([parts[0], moved[1], moved[2], moved[3]])
    got = lax.ppermute(sent, "zl", [(0, 1), (1, 0)])
    turned, kept = lax.optimization_barrier((turned, kept))
    triangle_inputs, edge_bias = triangle_stage(
        turned, triangle_proj, jnp.transpose(triangle_bias)
    )
    norm_own, edge_bias = lax.optimization_barrier((norm_own, edge_bias))
    alignment_update = combine_stage(
        kept, got, norm_own, average_gate, jnp.transpose(average_out)
    )
    return (pair_new, alignment_update, triangle_inputs, edge_bias)


def solution(mesh):
    fine = Mesh(mesh.devices.reshape(4, 4, 2, 2, 4), ALL)
    placed = (P(None, COL + ROW, None), P(ROW, COL, None)) + (P(),) * 10
    return jax.shard_map(
        per_device,
        mesh=fine,
        in_specs=placed,
        out_specs=(
            P(ROW, COL, None),
            P(None, ROW + COL, None),
            P(COL + ROW, None, None),
            P(None, COL + ROW, None),
        ),
        check_vma=False,
    )
```
